256 devices in a mesh: fsdp: 64 (over y, z, x_lo), tp: 4 (over x_hi, core).
Axes of the slice: x: 4 (x_hi: 2, x_lo: 2; x = x_hi * 2 + x_lo), y: 4, z: 8, core: 2. Of those that a mesh axis runs over, the one named last changes fastest.
Arguments:
- tokens: bfloat16 [24576, 5632], P('fsdp', 'tp'), may hold values from -6 to 6
- gain: float32 [5632], replicated, may hold values from 0.1 to 1.9
- query_projection_weight: bfloat16 [5632, 6144], P('fsdp', 'tp'), may hold values from -0.078125 to 0.078125
- key_projection_weight: bfloat16 [5632, 1024], P('fsdp', 'tp'), may hold values from -0.078125 to 0.078125
- value_projection_weight: bfloat16 [5632, 1024], P('fsdp', 'tp'), may hold values from -0.078125 to 0.078125
- adapter_down_factors: bfloat16 [3, 16, 5632], replicated, may hold values from -0.078125 to 0.078125
- query_adapter_up: bfloat16 [16, 6144], P(None, 'tp'), may hold values from -0.078125 to 0.078125
- key_adapter_up: bfloat16 [16, 1024], P(None, 'tp'), may hold values from -0.1875 to 0.1875
- value_adapter_up: bfloat16 [16, 1024], P(None, 'tp'), may hold values from -0.1875 to 0.1875
- query_cotangent: bfloat16 [24576, 6144], P('fsdp', 'tp'), may hold values from -6 to 6
- key_cotangent: bfloat16 [24576, 1024], P('fsdp', 'tp'), may hold values from -6 to 6
- value_cotangent: bfloat16 [24576, 1024], P('fsdp', 'tp'), may hold values from -6 to 6
Outputs:
- grad_tokens: bfloat16 [24576, 5632], P('fsdp', 'tp')
- grad_down: float32 [3, 16, 5632], P(None, None, 'tp')
- grad_up_query: float32 [16, 6144], P(None, 'tp')
- grad_up_key: float32 [16, 1024], P(None, 'tp')
- grad_up_value: float32 [16, 1024], P(None, 'tp')
The draws below stay inside these ranges and needn't reach their ends.
All inputs are finite; a program needn't handle non-finite values.
Results may differ from the reference program's by a relative error of at most 0.0096.
Values may be sent and summed in bfloat16 or wider, within the bound.
A program may use at most 128 MiB of HBM per device.

```python
import math
import jax
import jax.numpy as jnp
from jax import lax

MODEL_WIDTH = 5632
ADAPTER_RANK = 16
QUERY_WIDTH = 6144
KEY_VALUE_WIDTH = 1024
TOKEN_TOTAL = 24576


def steps_of(stream_key, dims, pieces, low, largest):
    factor_of = 1.0
    for dim, blocks in pieces:
        draws = jax.random.uniform(jax.random.fold_in(jax.random.fold_in(stream_key, 6), dim), (blocks,), jnp.float32, low / len(pieces), largest / len(pieces))
        factor_of = factor_of * jnp.repeat(jnp.exp(draws), dims[dim] // blocks).reshape((-1,) + (1,) * (len(dims) - 1 - dim))
    return factor_of


def scatter_about(key, extent, scale, most, split=(), kind=jnp.bfloat16):
    level = steps_of(key, extent, split, -0.22, 0.18) if split else 1.0
    drawn = jax.random.normal(key, extent, jnp.float32) * scale * level
    return jnp.minimum(jnp.maximum(drawn, -most), most).astype(kind)


def setup_inputs(seed: int = 0) -> dict:
    splits = jax.random.split(jax.random.key(seed), 13)
    return {
        "tokens": scatter_about(splits[0], (TOKEN_TOTAL, MODEL_WIDTH), 1.0, 6.0, ((0, 64), (1, 4))),
        "gain": jnp.clip(1.0 + 0.18 * jax.random.normal(splits[1], (MODEL_WIDTH,), jnp.float32), 0.1, 1.9),
        "query_projection_weight": scatter_about(splits[2], (MODEL_WIDTH, QUERY_WIDTH), MODEL_WIDTH ** -0.5, 0.078125, ((0, 64), (1, 4))),
        "key_projection_weight": scatter_about(splits[3], (MODEL_WIDTH, KEY_VALUE_WIDTH), MODEL_WIDTH ** -0.5, 0.078125, ((0, 64), (1, 4))),
        "value_projection_weight": scatter_about(splits[4], (MODEL_WIDTH, KEY_VALUE_WIDTH), MODEL_WIDTH ** -0.5, 0.078125, ((0, 64), (1, 4))),
        "adapter_down_factors": scatter_about(splits[5], (3, ADAPTER_RANK, MODEL_WIDTH), MODEL_WIDTH ** -0.5, 0.078125),
        "query_adapter_up": scatter_about(splits[6], (ADAPTER_RANK, QUERY_WIDTH), QUERY_WIDTH ** -0.5, 0.078125, ((1, 4),)),
        "key_adapter_up": scatter_about(splits[7], (ADAPTER_RANK, KEY_VALUE_WIDTH), KEY_VALUE_WIDTH ** -0.5, 0.1875, ((1, 4),)),
        "value_adapter_up": scatter_about(splits[8], (ADAPTER_RANK, KEY_VALUE_WIDTH), KEY_VALUE_WIDTH ** -0.5, 0.1875, ((1, 4),)),
        "query_cotangent": scatter_about(splits[9], (TOKEN_TOTAL, QUERY_WIDTH), 1.0, 6.0, ((0, 64), (1, 4))),
        "key_cotangent": scatter_about(splits[10], (TOKEN_TOTAL, KEY_VALUE_WIDTH), 1.0, 6.0, ((0, 64), (1, 4))),
        "value_cotangent": scatter_about(splits[11], (TOKEN_TOTAL, KEY_VALUE_WIDTH), 1.0, 6.0, ((0, 64), (1, 4))),
    }


norm_eps = 1e-05
adapter_scale = 2.0

def reference(tokens, gain, query_projection_weight, key_projection_weight, value_projection_weight, adapter_down_factors, query_adapter_up, key_adapter_up, value_adapter_up, query_cotangent, key_cotangent, value_cotangent):
    weights = (query_projection_weight, key_projection_weight, value_projection_weight)
    adapter_up_factors = (query_adapter_up, key_adapter_up, value_adapter_up)
    cotangent_list = (query_cotangent, key_cotangent, value_cotangent)
    token_width_matrix = tokens.astype(jnp.float32)
    inverse_root_mean = lax.rsqrt(lax.optimization_barrier(jnp.mean(token_width_matrix * token_width_matrix, axis=1, keepdims=True)) + norm_eps)
    unit_rows = token_width_matrix * inverse_root_mean
    scaled_input = unit_rows * gain[None, :]
    normed = scaled_input.astype(jnp.bfloat16)
    adapter_input = jnp.stack([jnp.dot(scaled_input, adapter_down_factors[slice_member].astype(jnp.float32).T, precision=lax.Precision.HIGHEST) for slice_member in range(3)])
    adapter_output = jnp.stack([jnp.dot(cotangent_list[slice_member], adapter_up_factors[slice_member].T, preferred_element_type=jnp.float32) for slice_member in range(3)])
    input_lowrank = adapter_input.astype(jnp.bfloat16)
    output_lowrank = adapter_output.astype(jnp.bfloat16)
    gradient_scale = adapter_scale / math.sqrt(TOKEN_TOTAL)
    backward_result = jnp.zeros(tokens.shape, jnp.float32)
    for slice_member in range(3):
        backward_result = backward_result + jnp.dot(cotangent_list[slice_member], weights[slice_member].T, preferred_element_type=jnp.float32)
    for slice_member in range(3):
        backward_result = backward_result + adapter_scale * jnp.dot(output_lowrank[slice_member], adapter_down_factors[slice_member], preferred_element_type=jnp.float32)
    gained = gain[None, :] * backward_result
    inner = lax.optimization_barrier(jnp.mean(gained * unit_rows, axis=1, keepdims=True))
    grad_tokens = (inverse_root_mean * (gained - unit_rows * inner)).astype(jnp.bfloat16)
    grad_down = jnp.stack([gradient_scale * jnp.dot(output_lowrank[slice_member].T, normed, preferred_element_type=jnp.float32) for slice_member in range(3)])
    grad_ups = [gradient_scale * jnp.dot(input_lowrank[slice_member].T, cotangent_list[slice_member], preferred_element_type=jnp.float32) for slice_member in range(3)]
    return (grad_tokens, grad_down, grad_ups[0], grad_ups[1], grad_ups[2])
```

```python
import functools
import heapq
import math

import jax
import jax.numpy as jnp
from jax import lax
from jax.experimental import pallas as pl
from jax.experimental.pallas import tpu as pltpu
from jax.sharding import PartitionSpec as P

norm_eps = 1e-05
adapter_scale = 2.0

MESH = pl.DeviceIdType.MESH
NY, NZ = 4, 8
SLOT = 48
CHUNKS = (8, 8, 8, 8, 8, 8, 8, 4, 4)


def forwards(have, item):
    part, dy, dz, half = item
    out = []
    if part == 0:
        if dz == 0:
            if dy == 0:
                out += [("y+", (0, 1, 0, None)), ("y-", (0, -1, 0, None))]
            elif dy == 1:
                out += [("y+", (0, 2, 0, 0))]
            elif dy == -1:
                out += [("y-", (0, 2, 0, 1))]
            if half is None or (0, 2, 0, 1 - half) in have:
                out += [("z+", (0, dy, 1, None)), ("z-", (0, dy, -1, None))]
        elif dz > 0:
            if dz < 3 or (dz == 3 and dy in (0, 1)):
                out += [("z+", (0, dy, dz + 1, None))]
        elif dz > -3:
            out += [("z-", (0, dy, dz - 1, None))]
        elif dy in (-1, 2):
            out += [("z-", (0, dy, 4, None))]
    elif dy == 0:
        if dz == 0:
            out += [("z+", (1, 0, 1, None)), ("z-", (1, 0, -1, None))]
        elif 0 < dz < 4:
            out += [("z+", (1, 0, dz + 1, 0 if dz == 3 else None))]
        elif dz < 0:
            out += [("z-", (1, 0, 4 if dz == -3 else dz - 1, 1 if dz == -3 else None))]
        if half is None or (1, 0, 4, 1 - half) in have:
            out += [("y+", (1, 1, dz, None)), ("y-", (1, -1, dz, None))]
    elif dy == 1 and dz in (0, 1, 2, 3):
        out += [("y+", (1, 2, dz, None))]
    elif dy == -1 and dz in (-1, -2, -3, 4):
        out += [("y-", (1, 2, dz, None))]
    return out


def gather_plan(rows, rate=44.0, latency=1.9):
    size = [r * 4.096 for r in rows]
    free = dict.fromkeys(("y+", "y-", "z+", "z-"), 0.0)
    have, events, log = set(), [], []

    def issue(now, link, item):
        span = size[item[0]] * (1.0 if item[3] is None else 0.5) / rate
        free[link] = max(now, free[link]) + span
        heapq.heappush(events, (free[link] + latency, len(log) + len(events), link, item))

    first = []
    for item in ((0, 0, 0, None), (1, 0, 0, None)):
        have.add(item)
        first += forwards(have, item)
    first = [e for e in first if e[0][0] == "y"] + [e for e in reversed(first) if e[0][0] == "z"]
    for link, item in first:
        issue(0.0, link, item)
    count = len(first)
    while events:
        now, _, link, item = heapq.heappop(events)
        have.add(item)
        onward = forwards(have, item)
        log.append((now, item, onward))
        for link, new in onward:
            issue(now + 0.1, link, new)
    slots = {(0, 0, 0): 0, (1, 0, 0): 1}
    whole = []
    for index, (now, item, _) in enumerate(log):
        key = item[:3]
        if item[3] is None or (*key, 1 - item[3]) in [e[1] for e in log[:index]]:
            slots[key] = len(slots)
            whole.append(index)
    return first, [(item, onward) for _, item, onward in log], slots


def gather_multiply_kernel(
    rows, wq, wk, wv, gq, gk, gv, out, wbuf, gbuf, keep, csend, crecv, xs, xr,
    load_sem, wsend_sem, wrecv_sem, g_sem, csend_sem, crecv_sem, xsend_sem, xrecv_sem,
):
    f = lax.axis_index("fsdp")
    t = lax.axis_index("tp")
    y, z, x_lo = f // 16, (f // 2) % 8, f % 2
    x_hi, core = t // 2, t % 2
    tokens = gq.shape[0]
    first, log, slots = gather_plan(rows)
    where = {v: k for k, v in slots.items()}

    def place(yy, zz, xx):
        return (yy % NY) * 16 + (zz % NZ) * 2 + xx

    link_device = {
        "y+": (place(y + 1, z, x_lo), t),
        "y-": (place(y + NY - 1, z, x_lo), t),
        "z+": (place(y, z + 1, x_lo), t),
        "z-": (place(y, z + NZ - 1, x_lo), t),
    }
    mate = (place(y, z, 1 - x_lo), t)
    twin = (f, x_hi * 2 + 1 - core)

    loads = []
    own_half = (x_lo + core) % 2
    own_rows = pl.ds(pl.multiple_of(own_half * tokens, 128), tokens)
    column = 0
    for index, (w, g) in enumerate(((wq, gq), (wk, gk), (wv, gv))):
        width = w.shape[1]
        columns = pl.ds(column, width)
        loads.append(pltpu.make_async_copy(w.at[pl.ds(0, rows[0])], wbuf.at[0, pl.ds(0, rows[0]), columns], load_sem.at[3 * index]))
        loads.append(pltpu.make_async_copy(w.at[pl.ds(rows[0], rows[1])], wbuf.at[1, pl.ds(0, rows[1]), columns], load_sem.at[3 * index + 1]))
        loads.append(pltpu.make_async_copy(g, gbuf.at[own_rows, columns], load_sem.at[3 * index + 2]))
        column += width
    for load in loads:
        load.start()

    barrier = pltpu.get_barrier_semaphore()
    partners = list(link_device.values())
    for dhi in (0, 1):
        for dlo in (0, 1):
            for dc in (0, 1):
                if dhi or dlo or dc:
                    partners.append((place(y, z, (x_lo + dlo) % 2), ((x_hi + dhi) % 2) * 2 + (core + dc) % 2))
    for device in partners:
        pl.semaphore_signal(barrier, inc=1, device_id=device, device_id_type=MESH)
    pl.semaphore_wait(barrier, len(partners))
    for load in loads:
        load.wait()

    g_copy = pltpu.make_async_remote_copy(
        src_ref=gbuf.at[own_rows], dst_ref=gbuf.at[own_rows], send_sem=g_sem.at[0], recv_sem=g_sem.at[1],
        device_id=mate, device_id_type=MESH,
    )

    event_index = {item: index for index, (item, _) in enumerate(log)}
    half_width = wbuf.shape[2] // 2
    sends = []

    def block(item):
        part, dy, dz, half = item
        ref = wbuf.at[slots[(part, dy, dz)], pl.ds(0, rows[part])]
        if half is not None:
            ref = wbuf.at[slots[(part, dy, dz)], pl.ds(0, rows[part]), pl.ds(half * half_width, half_width)]
        return ref

    def source(item, have):
        return item

    def send(origin, link, item):
        part, dy, dz, half = item
        src = wbuf.at[slots[origin[:3]], pl.ds(0, rows[part])]
        if half is not None:
            src = wbuf.at[slots[origin[:3]], pl.ds(0, rows[part]), pl.ds(half * half_width, half_width)]
        index = event_index[item]
        copy = pltpu.make_async_remote_copy(
            src_ref=src, dst_ref=block(item), send_sem=wsend_sem.at[index], recv_sem=wrecv_sem.at[index],
            device_id=link_device[link], device_id_type=MESH,
        )
        copy.start()
        sends.append(copy)

    for link, item in first:
        send((item[0], 0, 0, None), link, item)
    g_copy.start()

    starts = [sum(CHUNKS[:k]) for k in range(len(CHUNKS))]
    core_copies = {}
    same = x_lo == core
    my_chip = x_hi * 2 + x_lo

    def multiply(k):
        begin, count = starts[k], CHUNKS[k]
        lines = wbuf[begin : begin + count].reshape(count * SLOT, wbuf.shape[2])
        product = lax.dot_general(lines, gbuf[...], (((1,), (1,)), ((), ())), preferred_element_type=jnp.float32)
        keep[begin * SLOT : (begin + count) * SLOT, :] = product[:, :tokens]
        csend[begin : begin + count] = product[:, tokens:].astype(jnp.bfloat16).reshape(count, SLOT, tokens)
        copy = pltpu.make_async_remote_copy(
            src_ref=csend.at[pl.ds(begin, count)], dst_ref=crecv.at[pl.ds(begin, count)],
            send_sem=csend_sem.at[k], recv_sem=crecv_sem.at[k], device_id=twin, device_id_type=MESH,
        )
        copy.start()
        core_copies[k] = copy

    def pass_on(k):
        begin, count = starts[k], CHUNKS[k]
        core_copies[k].wait_recv()
        total = keep[begin * SLOT : (begin + count) * SLOT, :] + crecv[begin : begin + count].reshape(count * SLOT, tokens).astype(jnp.float32)
        xs[begin : begin + count] = total.astype(jnp.bfloat16).reshape(count, SLOT, tokens)
        for slot in range(begin, begin + count):
            part, dy, dz = where[slot]
            owner_y, owner_z = (y + NY - dy) % NY, (z + NZ - dz) % NZ
            src = xs.at[slot, pl.ds(0, rows[part])]
            dst = xr.at[my_chip, owner_z, pl.ds(part * rows[0], rows[part])]
            own = jnp.logical_and(same, owner_y == t)

            @pl.when(own)
            def _():
                pltpu.make_async_copy(src, dst, xrecv_sem.at[my_chip]).start()

            @pl.when(jnp.logical_not(own))
            def _():
                pltpu.make_async_remote_copy(
                    src_ref=src, dst_ref=dst, send_sem=xsend_sem, recv_sem=xrecv_sem.at[my_chip],
                    device_id=(place(y, z, core), owner_y), device_id_type=MESH,
                ).start()

    done_slots, done_chunks, passed = 2, 0, 0
    have = {(0, 0, 0, None), (1, 0, 0, None)}
    g_waited = False
    for index, (item, onward) in enumerate(log):
        pltpu.make_async_copy(block(item), block(item), wrecv_sem.at[index]).wait()
        have.add(item)
        for link, new in onward:
            send(item, link, new)
        if item[3] is None or (*item[:3], 1 - item[3]) in have:
            done_slots += 1
        if done_chunks >= 1 and passed < done_chunks and (index % 2 == 0):
            pass
        while done_chunks < len(CHUNKS) and starts[done_chunks] + CHUNKS[done_chunks] <= done_slots and index >= 31:
            if not g_waited:
                g_copy.wait_recv()
                g_waited = True
            multiply(done_chunks)
            done_chunks += 1
            if done_chunks - passed > 1:
                pass_on(passed)
                passed += 1
            if index < len(log) - 1:
                break
    while passed < len(CHUNKS):
        pass_on(passed)
        passed += 1
    for chip in range(4):
        pltpu.make_async_copy(xr.at[chip], xr.at[chip], xrecv_sem.at[chip]).wait()
    for half in range(2):
        out[:, half] = xr[half].astype(jnp.float32) + xr[2 + half].astype(jnp.float32)

    g_copy.wait_send()
    for copy in sends:
        copy.wait_send()
    for copy in core_copies.values():
        copy.wait_send()

    @pl.when(same)
    def _():
        pltpu.make_async_copy(xr.at[pl.ds(0, 3)], xr.at[pl.ds(0, 3)], xsend_sem).wait()

    @pl.when(jnp.logical_not(same))
    def _():
        pltpu.make_async_copy(xr, xr, xsend_sem).wait()


def gather_multiply(weights, cotangents):
    tokens = cotangents[0].shape[0]
    owned = weights[0].shape[0]
    rows = (40, owned - 40)
    width = sum(w.shape[1] for w in weights)
    events = len(gather_plan(rows)[1])
    slots = 2 * NY * NZ
    chunks = len(CHUNKS)
    bf16 = jnp.bfloat16
    return pl.pallas_call(
        functools.partial(gather_multiply_kernel, rows),
        out_shape=jax.ShapeDtypeStruct((NZ, 2, owned, tokens), jnp.float32),
        in_specs=[pl.BlockSpec(memory_space=pl.ANY)] * 6,
        out_specs=pl.BlockSpec(memory_space=pltpu.VMEM),
        scratch_shapes=[
            pltpu.VMEM((slots, SLOT, width), bf16),
            pltpu.VMEM((2 * tokens, width), bf16),
            pltpu.VMEM((slots * SLOT, tokens), jnp.float32),
            pltpu.VMEM((slots, SLOT, tokens), bf16),
            pltpu.VMEM((slots, SLOT, tokens), bf16),
            pltpu.VMEM((slots, SLOT, tokens), bf16),
            pltpu.VMEM((4, NZ, owned, tokens), bf16),
            pltpu.SemaphoreType.DMA((9,)),
            pltpu.SemaphoreType.DMA((events,)),
            pltpu.SemaphoreType.DMA((events,)),
            pltpu.SemaphoreType.DMA((2,)),
            pltpu.SemaphoreType.DMA((chunks,)),
            pltpu.SemaphoreType.DMA((chunks,)),
            pltpu.SemaphoreType.DMA,
            pltpu.SemaphoreType.DMA((4,)),
        ],
        compiler_params=pltpu.CompilerParams(collective_id=0, has_side_effects=True, vmem_limit_bytes=52 << 20),
        cost_estimate=pl.CostEstimate(flops=9 * 10**9, bytes_accessed=6 * 10**6, transcendentals=0),
        name="gather_multiply",
    )(*weights, *cotangents)


def from_everyone(array, axis):
    copies = jnp.broadcast_to(array, (lax.axis_size(axis), *array.shape))
    return lax.all_to_all(copies, axis, split_axis=0, concat_axis=0, tiled=True)


def over_copies(array, axis):
    return from_everyone(array, axis).sum(axis=0)


def in_one(arrays, axis, total_of):
    ends = [0]
    for a in arrays:
        ends.append(ends[-1] + a.size)
    total = total_of(jnp.concatenate([a.ravel() for a in arrays]), axis)
    return tuple((total[b:e].reshape(a.shape) for a, b, e in zip(arrays, ends, ends[1:])))


def shards(
    tokens,
    gain,
    query_projection_weight,
    key_projection_weight,
    value_projection_weight,
    adapter_down_factors,
    query_adapter_up,
    key_adapter_up,
    value_adapter_up,
    query_cotangent,
    key_cotangent,
    value_cotangent,
):
    adapter_up_factors = (query_adapter_up, key_adapter_up, value_adapter_up)
    cotangent_list = (query_cotangent, key_cotangent, value_cotangent)
    tensor_slice_index = lax.axis_index("tp")
    number_of_rows, owned_width = tokens.shape
    full_width = gain.shape[0]
    token_width_matrix = tokens.astype(jnp.float32)
    gain_own = lax.dynamic_slice_in_dim(gain, tensor_slice_index * owned_width, owned_width, 0)
    down_owned_slice = lax.dynamic_slice_in_dim(
        adapter_down_factors, tensor_slice_index * owned_width, owned_width, 2
    )
    scaled_part = token_width_matrix * gain_own[None, :]
    adapter_input_slice = jnp.einsum(
        "td,krd->ktr",
        scaled_part,
        down_owned_slice.astype(jnp.float32),
        precision=lax.Precision.HIGHEST,
    )
    adapter_output_slice = jnp.stack(
        [
            jnp.dot(
                cotangent_list[slice_member],
                adapter_up_factors[slice_member].T,
                preferred_element_type=jnp.float32,
            )
            for slice_member in range(3)
        ]
    )
    squared_total, adapter_input_unnormed, adapter_output = in_one(
        (
            jnp.sum(token_width_matrix * token_width_matrix, axis=1),
            adapter_input_slice,
            adapter_output_slice,
        ),
        "tp",
        over_copies,
    )
    inverse_root_mean = lax.rsqrt(squared_total / full_width + norm_eps)[:, None]
    adapter_input = adapter_input_unnormed * inverse_root_mean[None]
    unit_rows = token_width_matrix * inverse_root_mean
    normed = (unit_rows * gain_own[None, :]).astype(jnp.bfloat16)
    input_lowrank = adapter_input.astype(jnp.bfloat16)
    output_lowrank = adapter_output.astype(jnp.bfloat16)
    gradient_scale = adapter_scale / math.sqrt(number_of_rows * lax.axis_size("fsdp"))
    down_local = gradient_scale * jnp.einsum(
        "ktr,td->krd", output_lowrank, normed, preferred_element_type=jnp.float32
    )
    up_local = tuple(
        (
            gradient_scale
            * jnp.dot(
                input_lowrank[slice_member].T,
                cotangent_list[slice_member],
                preferred_element_type=jnp.float32,
            )
            for slice_member in range(3)
        )
    )
    grad_down, grad_up_query, grad_up_key, grad_up_value = in_one(
        (down_local, up_local[0], up_local[1], up_local[2]), "fsdp", lax.psum
    )
    back_t = gather_multiply(
        (query_projection_weight, key_projection_weight, value_projection_weight), cotangent_list
    )
    backward_result = back_t.reshape(owned_width, number_of_rows).T
    backward_result = backward_result + adapter_scale * jnp.einsum(
        "ktr,krd->td", output_lowrank, down_owned_slice, preferred_element_type=jnp.float32
    )
    gained = gain_own[None, :] * backward_result
    inner = over_copies(jnp.sum(gained * unit_rows, axis=1), "tp") / full_width
    grad_tokens = (inverse_root_mean * (gained - unit_rows * inner[:, None])).astype(jnp.bfloat16)
    return (grad_tokens, grad_down, grad_up_query, grad_up_key, grad_up_value)


def solution(mesh):
    in_specs = (
        P("fsdp", "tp"),
        P(),
        P("fsdp", "tp"),
        P("fsdp", "tp"),
        P("fsdp", "tp"),
        P(),
        P(None, "tp"),
        P(None, "tp"),
        P(None, "tp"),
        P("fsdp", "tp"),
        P("fsdp", "tp"),
        P("fsdp", "tp"),
    )
    out_specs = (P("fsdp", "tp"), P(None, None, "tp"), P(None, "tp"), P(None, "tp"), P(None, "tp"))
    return jax.shard_map(shards, mesh=mesh, in_specs=in_specs, out_specs=out_specs, check_vma=False)
```

```python
import functools
import heapq
import math

import jax
import jax.numpy as jnp
from jax import lax
from jax.experimental import pallas as pl
from jax.experimental.pallas import tpu as pltpu
from jax.sharding import PartitionSpec as P

norm_eps = 1e-05
adapter_scale = 2.0

MESH = pl.DeviceIdType.MESH
NY, NZ = 4, 8
SLOT = 48
CHUNKS = (8, 8, 8, 8, 8, 8, 8, 4, 4)
G_PIECES = 4
G_EVENT = 33


def forwards(have, item):
    part, dy, dz, half = item
    out = []
    if part == 0:
        if dz == 0:
            if dy == 0:
                out += [("y+", (0, 1, 0, None)), ("y-", (0, -1, 0, None))]
            elif dy == 1:
                out += [("y+", (0, 2, 0, 0))]
            elif dy == -1:
                out += [("y-", (0, 2, 0, 1))]
            if half is None or (0, 2, 0, 1 - half) in have:
                out += [("z+", (0, dy, 1, None)), ("z-", (0, dy, -1, None))]
        elif dz > 0:
            if dz < 3 or (dz == 3 and dy in (0, 1)):
                out += [("z+", (0, dy, dz + 1, None))]
        elif dz > -3:
            out += [("z-", (0, dy, dz - 1, None))]
        elif dy in (-1, 2):
            out += [("z-", (0, dy, 4, None))]
    elif dy == 0:
        if dz == 0:
            out += [("z+", (1, 0, 1, None)), ("z-", (1, 0, -1, None))]
        elif 0 < dz < 4:
            out += [("z+", (1, 0, dz + 1, 0 if dz == 3 else None))]
        elif dz < 0:
            out += [("z-", (1, 0, 4 if dz == -3 else dz - 1, 1 if dz == -3 else None))]
        if half is None or (1, 0, 4, 1 - half) in have:
            out += [("y+", (1, 1, dz, None)), ("y-", (1, -1, dz, None))]
    elif dy == 1 and dz in (0, 1, 2, 3):
        out += [("y+", (1, 2, dz, None))]
    elif dy == -1 and dz in (-1, -2, -3, 4):
        out += [("y-", (1, 2, dz, None))]
    return out


def gather_plan(rows, rate=44.0, latency=1.9):
    size = [r * 4.096 for r in rows]
    free = dict.fromkeys(("y+", "y-", "z+", "z-"), 0.0)
    have, events, log = set(), [], []

    def issue(now, link, item):
        span = size[item[0]] * (1.0 if item[3] is None else 0.5) / rate
        free[link] = max(now, free[link]) + span
        heapq.heappush(events, (free[link] + latency, len(log) + len(events), link, item))

    first = []
    for item in ((0, 0, 0, None), (1, 0, 0, None)):
        have.add(item)
        first += forwards(have, item)
    first = [e for e in first if e[0][0] == "y"] + [e for e in reversed(first) if e[0][0] == "z"]
    for link, item in first:
        issue(0.0, link, item)
    count = len(first)
    while events:
        now, _, link, item = heapq.heappop(events)
        have.add(item)
        onward = forwards(have, item)
        log.append((now, item, onward))
        for link, new in onward:
            issue(now + 0.1, link, new)
    slots = {(0, 0, 0): 0, (1, 0, 0): 1}
    whole = []
    for index, (now, item, _) in enumerate(log):
        key = item[:3]
        if item[3] is None or (*key, 1 - item[3]) in [e[1] for e in log[:index]]:
            slots[key] = len(slots)
            whole.append(index)
    return first, [(item, onward) for _, item, onward in log], slots


def dot_nt(a, b):
    return lax.dot_general(a, b, (((1,), (1,)), ((), ())), preferred_element_type=jnp.float32)


def as_column(row):
    return jnp.transpose(jnp.broadcast_to(row, (128, row.shape[1])))[:, :1]


def layer_kernel(
    rows, wq, wk, wv, gq, gk, gv, tokens_hbm, gain_all, down_all, uq, uk, uv,
    grad, down_out, upq_out, upk_out, upv_out,
    wbuf, gbuf, keep, csend, crecv, xs, xr,
    tok, tok_t, acc, turned, gain_column, low, low_total, out_low_buf, inverse, inner_buf,
    arw, ar1, ar2, ar3, arg,
    load_sem, wsend_sem, wrecv_sem, gsend_sem, grecv_sem, csend_sem, crecv_sem, xsend_sem, xrecv_sem,
    lsend_sem, lrecv_sem, asend_sem, arecv_sem, isend_sem, irecv_sem,
):
    f = lax.axis_index("fsdp")
    t = lax.axis_index("tp")
    y, z, x_lo = f // 16, (f // 2) % 8, f % 2
    x_hi, core = t // 2, t % 2
    tokens, owned_width = tokens_hbm.shape
    full_width = gain_all.shape[1]
    f32, bf16 = jnp.float32, jnp.bfloat16
    first, log, slots = gather_plan(rows)
    where = {v: k for k, v in slots.items()}

    def place(yy, zz, xx):
        return (yy % NY) * 16 + (zz % NZ) * 2 + xx

    link_device = {
        "y+": (place(y + 1, z, x_lo), t),
        "y-": (place(y + NY - 1, z, x_lo), t),
        "z+": (place(y, z + 1, x_lo), t),
        "z-": (place(y, z + NZ - 1, x_lo), t),
    }
    mate = (place(y, z, 1 - x_lo), t)
    twin = (f, x_hi * 2 + 1 - core)
    across = (f, (1 - x_hi) * 2 + core)

    def remote(src, dst, send_sem, recv_sem, device):
        return pltpu.make_async_remote_copy(
            src_ref=src, dst_ref=dst, send_sem=send_sem, recv_sem=recv_sem, device_id=device, device_id_type=MESH
        )

    def landed(ref, sem):
        pltpu.make_async_copy(ref, ref, sem).wait()

    started = []

    def send_now(*args):
        copy = remote(*args)
        copy.start()
        started.append(copy)
        return copy

    loads, token_load = [], pltpu.make_async_copy(tokens_hbm, tok, load_sem.at[9])
    own_half = (x_lo + core) % 2
    own_begin = pl.multiple_of(own_half * tokens, 128)
    column, spans = 0, []
    for index, (w, g) in enumerate(((wq, gq), (wk, gk), (wv, gv))):
        width = w.shape[1]
        columns = pl.ds(column, width)
        spans.append((column, width))
        loads.append(pltpu.make_async_copy(w.at[pl.ds(0, rows[0])], wbuf.at[0, pl.ds(0, rows[0]), columns], load_sem.at[3 * index]))
        loads.append(pltpu.make_async_copy(w.at[pl.ds(rows[0], rows[1])], wbuf.at[1, pl.ds(0, rows[1]), columns], load_sem.at[3 * index + 1]))
        column += width
    for index, g in enumerate((gq, gk, gv)):
        columns = pl.ds(*spans[index])
        loads.append(pltpu.make_async_copy(g, gbuf.at[pl.ds(own_begin, tokens), columns], load_sem.at[3 * index + 2]))
    for load in loads:
        load.start()
    token_load.start()

    barrier = pltpu.get_barrier_semaphore()
    partners = [(place(y + k, z, x_lo), t) for k in range(1, NY)] + [(place(y, z + k, x_lo), t) for k in range(1, NZ)]
    for dhi in (0, 1):
        for dlo in (0, 1):
            for dc in (0, 1):
                if dhi or dlo or dc:
                    partners.append((place(y, z, (x_lo + dlo) % 2), ((x_hi + dhi) % 2) * 2 + (core + dc) % 2))
    for device in partners:
        pl.semaphore_signal(barrier, inc=1, device_id=device, device_id_type=MESH)
    pl.semaphore_wait(barrier, len(partners))
    for load in loads:
        load.wait()

    event_index = {item: index for index, (item, _) in enumerate(log)}
    half_width = wbuf.shape[2] // 2

    def block(slot, part, half):
        if half is None:
            return wbuf.at[slot, pl.ds(0, rows[part])]
        return wbuf.at[slot, pl.ds(0, rows[part]), pl.ds(half * half_width, half_width)]

    def forward(origin, link, item):
        part, half, index = item[0], item[3], event_index[item]
        send_now(
            block(slots[origin[:3]], part, half), block(slots[item[:3]], part, half),
            wsend_sem.at[index], wrecv_sem.at[index], link_device[link],
        )

    for link, item in first:
        forward((item[0], 0, 0), link, item)

    g_lines = tokens // G_PIECES

    def g_piece(k):
        return gbuf.at[pl.ds(pl.multiple_of(own_half * tokens + k * g_lines, 32), g_lines)]

    def g_send(k):
        send_now(g_piece(k), g_piece(k), gsend_sem.at[k], grecv_sem.at[k], mate)

    def g_wait():
        for k in range(G_PIECES):
            landed(gbuf.at[pl.ds(0, g_lines)], grecv_sem.at[k])

    gain_row = gain_all[:, pl.ds(pl.multiple_of(t * owned_width, 128), owned_width)]
    down = down_all[:, pl.ds(pl.multiple_of(t * owned_width, 128), owned_width)]
    rank3, rank = down.shape[0], down.shape[0] // 3

    def low_products():
        token_load.wait()
        scaled = down.astype(f32) * gain_row
        high = scaled.astype(bf16)
        rest = scaled - high.astype(f32)
        middle = rest.astype(bf16)
        lowest = (rest - middle.astype(f32)).astype(bf16)
        lines = tok[...]
        for begin, part in ((0, high), (1, middle), (2, lowest)):
            term = dot_nt(part, lines)
            low[0, 0:rank3] = term if begin == 0 else low[0, 0:rank3] + term
        for m, up in enumerate((uq, uk, uv)):
            begin, width = spans[m]
            own = gbuf[pl.ds(own_begin, tokens), begin : begin + width]
            low[0, rank3 + m * rank : rank3 + (m + 1) * rank] = dot_nt(up[...], own)
        squares = lines.astype(f32) * lines.astype(f32)
        high = squares.astype(bf16)
        lowest = (squares - high.astype(f32)).astype(bf16)
        ones = jnp.ones((16, owned_width), bf16)
        low[0, 2 * rank3 : 2 * rank3 + 8] = (dot_nt(ones, high) + dot_nt(ones, lowest))[:8]
        send_now(low.at[0], low.at[1], lsend_sem.at[0], lrecv_sem.at[0], twin)

    def low_pair():
        landed(low.at[1], lrecv_sem.at[0])
        low[2] = low[0] + low[1]
        send_now(low.at[2], low.at[3], lsend_sem.at[1], lrecv_sem.at[1], across)

    gradient_scale = adapter_scale / math.sqrt(tokens * 64)

    def low_all():
        landed(low.at[3], lrecv_sem.at[1])
        low_total[...] = low[2] + low[3]
        inverse_row = lax.rsqrt(low_total[2 * rank3 : 2 * rank3 + 8] / full_width + norm_eps)
        inverse[...] = inverse_row
        in_low = (low_total[0:rank3] * inverse_row[:1]).astype(bf16)
        out_low = low_total[rank3 : 2 * rank3].astype(bf16)
        out_low_buf[...] = out_low
        unit = tok[...].astype(f32) * as_column(inverse_row[:1])
        normed = (unit * gain_row).astype(bf16)
        local = gradient_scale * jnp.dot(out_low, normed, preferred_element_type=f32)
        at = 0
        for j in range(owned_width // 128):
            arw[at : at + rank3] = local[:, j * 128 : (j + 1) * 128]
            at += rank3
        for m in range(3):
            begin, width = spans[m]
            own = gbuf[pl.ds(own_begin, tokens), begin : begin + width]
            local = gradient_scale * jnp.dot(in_low[m * rank : (m + 1) * rank], own, preferred_element_type=f32)
            for j in range(width // 128):
                arw[at : at + rank] = local[:, j * 128 : (j + 1) * 128]
                at += rank
        arw[at:] = jnp.zeros((arw.shape[0] - at, 128), f32)
        send_now(arw.at[pl.ds(pl.multiple_of((1 - x_lo) * 512, 16), 512)], ar1, asend_sem.at[0], arecv_sem.at[0], mate)

    def ar_rows(xx, yy=None, zz=None):
        if yy is None:
            return pl.ds(pl.multiple_of(xx * 512, 16), 512)
        if zz is None:
            return pl.ds(pl.multiple_of(xx * 512 + yy * 128, 16), 128)
        return pl.ds(pl.multiple_of(xx * 512 + yy * 128 + zz * 16, 16), 16)

    def sum_x():
        landed(ar1, arecv_sem.at[0])
        arw[ar_rows(x_lo)] = arw[ar_rows(x_lo)] + ar1[...]
        for k in range(1, NY):
            other = (y + k) % NY
            send_now(arw.at[ar_rows(x_lo, other)], ar2.at[k - 1], asend_sem.at[k], arecv_sem.at[k], (place(other, z, x_lo), t))

    def sum_y():
        for k in range(1, NY):
            landed(ar2.at[k - 1], arecv_sem.at[k])
        arw[ar_rows(x_lo, y)] = arw[ar_rows(x_lo, y)] + ar2[0] + ar2[1] + ar2[2]
        for k in range(1, NZ):
            other = (z + k) % NZ
            send_now(arw.at[ar_rows(x_lo, y, other)], ar3.at[k - 1], asend_sem.at[3 + k], arecv_sem.at[3 + k], (place(y, other, x_lo), t))

    def sum_z():
        for k in range(1, NZ):
            landed(ar3.at[k - 1], arecv_sem.at[3 + k])
        total = arw[ar_rows(x_lo, y, z)]
        for k in range(NZ - 1):
            total = total + ar3[k]
        arg[ar_rows(x_lo, y, z)] = total
        for k in range(1, NZ):
            mine = arg.at[ar_rows(x_lo, y, z)]
            send_now(mine, mine, asend_sem.at[10 + k], arecv_sem.at[10 + k], (place(y, z + k, x_lo), t))

    def spread_y():
        for k in range(1, NZ):
            landed(ar3.at[0], arecv_sem.at[10 + k])
        for k in range(1, NY):
            mine = arg.at[ar_rows(x_lo, y)]
            send_now(mine, mine, asend_sem.at[17 + k], arecv_sem.at[17 + k], (place(y + k, z, x_lo), t))

    def spread_x():
        for k in range(1, NY):
            landed(ar2.at[0], arecv_sem.at[17 + k])
        mine = arg.at[ar_rows(x_lo)]
        send_now(mine, mine, asend_sem.at[21], arecv_sem.at[21], mate)

    def adapter_outputs():
        landed(ar1, arecv_sem.at[21])
        at = 0
        for j in range(owned_width // 128):
            down_out[:, j * 128 : (j + 1) * 128] = arg[at : at + rank3]
            at += rank3
        for ref in (upq_out, upk_out, upv_out):
            for j in range(ref.shape[1] // 128):
                ref[:, j * 128 : (j + 1) * 128] = arg[at : at + rank]
                at += rank

    def columns_ready():
        gain_column[...] = jnp.transpose(jnp.broadcast_to(gain_row, (128, owned_width)))
        for j in range(owned_width // 128):
            tok_t[j * 128 : (j + 1) * 128] = jnp.transpose(tok[:, j * 128 : (j + 1) * 128].astype(f32))

    def adapter_term():
        acc[...] = adapter_scale * lax.dot_general(
            jnp.transpose(down.astype(f32)).astype(bf16), out_low_buf[...], (((1,), (0,)), ((), ())), preferred_element_type=f32
        )

    starts = [sum(CHUNKS[:k]) for k in range(len(CHUNKS))]
    core_copies = {}
    same = x_lo == core
    my_chip = x_hi * 2 + x_lo

    def multiply(k):
        begin, count = starts[k], CHUNKS[k]
        lines = wbuf[begin : begin + count].reshape(count * SLOT, wbuf.shape[2])
        product = dot_nt(lines, gbuf[...])
        keep[begin * SLOT : (begin + count) * SLOT, :] = product[:, :tokens]
        csend[begin : begin + count] = product[:, tokens:].astype(bf16).reshape(count, SLOT, tokens)
        both = pl.ds(begin, count)
        core_copies[k] = send_now(csend.at[both], crecv.at[both], csend_sem.at[k], crecv_sem.at[k], twin)

    def pass_on(k):
        begin, count = starts[k], CHUNKS[k]
        core_copies[k].wait_recv()
        got = crecv[begin : begin + count].reshape(count * SLOT, tokens).astype(f32)
        total = keep[begin * SLOT : (begin + count) * SLOT, :] + got
        xs[begin : begin + count] = total.astype(bf16).reshape(count, SLOT, tokens)
        for slot in range(begin, begin + count):
            part, dy, dz = where[slot]
            owner_y, owner_z = (y + NY - dy) % NY, (z + NZ - dz) % NZ
            src = xs.at[slot, pl.ds(0, rows[part])]
            dst = xr.at[my_chip, owner_z, pl.ds(part * rows[0], rows[part])]
            own = jnp.logical_and(same, owner_y == t)

            @pl.when(own)
            def _():
                pltpu.make_async_copy(src, dst, xrecv_sem.at[my_chip]).start()

            @pl.when(jnp.logical_not(own))
            def _():
                remote(src, dst, xsend_sem, xrecv_sem.at[my_chip], (place(y, z, core), owner_y)).start()

    TASKS = {
        -1: (functools.partial(g_send, 0), low_products),
        1: (low_pair, functools.partial(g_send, 1)),
        8: (low_all, functools.partial(g_send, 2)),
        9: (columns_ready,),
        10: (functools.partial(g_send, 3), adapter_term),
        21: (sum_x,),
        29: (sum_y,),
        37: (sum_z,),
        45: (spread_y,),
        53: (spread_x,),
    }

    for task in TASKS[-1]:
        task()
    done_slots, done_chunks, passed = 2, 0, 0
    have = {(0, 0, 0, None), (1, 0, 0, None)}
    g_waited = False
    for index, (item, onward) in enumerate(log):
        landed(block(slots[item[:3]], item[0], item[3]), wrecv_sem.at[index])
        have.add(item)
        for link, new in onward:
            forward(item, link, new)
        if item[3] is None or (*item[:3], 1 - item[3]) in have:
            done_slots += 1
        for task in TASKS.get(index, ()):
            task()
        while done_chunks < len(CHUNKS) and starts[done_chunks] + CHUNKS[done_chunks] <= done_slots and index >= G_EVENT:
            if not g_waited:
                g_wait()
                g_waited = True
            multiply(done_chunks)
            done_chunks += 1
            if done_chunks - passed > 1:
                pass_on(passed)
                passed += 1
            if index < len(log) - 1:
                break
    while passed < len(CHUNKS):
        pass_on(passed)
        passed += 1
    adapter_outputs()
    for chip in range(4):
        landed(xr.at[chip], xrecv_sem.at[chip])

    inverse_row = inverse[:1]
    inner = jnp.zeros((8, tokens), f32)
    for owner_z in range(NZ):
        for half in range(2):
            begin = (owner_z * 2 + half) * (rows[0] + rows[1])
            lines = pl.ds(begin, rows[0] + rows[1])
            back = xr[half, owner_z].astype(f32) + xr[2 + half, owner_z].astype(f32) + acc[lines]
            gained = gain_column[lines, :1] * back
            acc[lines] = gained
            product = gained * (tok_t[lines] * inverse_row)
            inner = inner + product.reshape(-1, 8, tokens).sum(axis=0)
    inner_buf[0] = inner
    for k, device in enumerate((twin, across, (f, (1 - x_hi) * 2 + 1 - core))):
        send_now(inner_buf.at[0], inner_buf.at[k + 1], isend_sem.at[k], irecv_sem.at[k], device)
    for j in range(owned_width // 128):
        turned[:, j * 128 : (j + 1) * 128] = jnp.transpose(acc[j * 128 : (j + 1) * 128])
    for k in range(3):
        landed(inner_buf.at[k + 1], irecv_sem.at[k])
    total = (inner_buf[0] + inner_buf[1]) + (inner_buf[2] + inner_buf[3])
    total = jnp.sum(total, axis=0, keepdims=True) / full_width
    inner_column, inverse_column = as_column(total), as_column(inverse_row)
    unit = tok[...].astype(f32) * inverse_column
    grad[...] = (inverse_column * (turned[...] - unit * inner_column)).astype(bf16)

    for copy in started:
        copy.wait_send()

    @pl.when(same)
    def _():
        landed(xr.at[pl.ds(0, 3)], xsend_sem)

    @pl.when(jnp.logical_not(same))
    def _():
        landed(xr, xsend_sem)


def layer(weights, cotangents, tokens, gain, down, ups):
    count, owned_width = tokens.shape
    owned = weights[0].shape[0]
    rows = (40, owned - 40)
    width = sum(w.shape[1] for w in weights)
    events = len(gather_plan(rows)[1])
    slots = 2 * NY * NZ
    chunks = len(CHUNKS)
    rank3 = down.shape[0]
    f32, bf16, dma = jnp.float32, jnp.bfloat16, pltpu.SemaphoreType.DMA
    vmem = pl.BlockSpec(memory_space=pltpu.VMEM)
    return pl.pallas_call(
        functools.partial(layer_kernel, rows),
        out_shape=(
            jax.ShapeDtypeStruct((count, owned_width), bf16),
            jax.ShapeDtypeStruct((rank3, owned_width), f32),
            *(jax.ShapeDtypeStruct(u.shape, f32) for u in ups),
        ),
        in_specs=[pl.BlockSpec(memory_space=pl.ANY)] * 7 + [vmem] * 5,
        out_specs=(vmem,) * 5,
        scratch_shapes=[
            pltpu.VMEM((slots, SLOT, width), bf16),
            pltpu.VMEM((2 * count, width), bf16),
            pltpu.VMEM((slots * SLOT, count), f32),
            pltpu.VMEM((slots, SLOT, count), bf16),
            pltpu.VMEM((slots, SLOT, count), bf16),
            pltpu.VMEM((slots, SLOT, count), bf16),
            pltpu.VMEM((4, NZ, owned, count), bf16),
            pltpu.VMEM((count, owned_width), bf16),
            pltpu.VMEM((owned_width, count), f32),
            pltpu.VMEM((owned_width, count), f32),
            pltpu.VMEM((count, owned_width), f32),
            pltpu.VMEM((owned_width, 128), f32),
            pltpu.VMEM((4, 2 * rank3 + 8, count), f32),
            pltpu.VMEM((2 * rank3 + 8, count), f32),
            pltpu.VMEM((rank3, count), bf16),
            pltpu.VMEM((8, count), f32),
            pltpu.VMEM((4, 8, count), f32),
            pltpu.VMEM((1024, 128), f32),
            pltpu.VMEM((512, 128), f32),
            pltpu.VMEM((3, 128, 128), f32),
            pltpu.VMEM((7, 16, 128), f32),
            pltpu.VMEM((1024, 128), f32),
            dma((10,)), dma((events,)), dma((events,)), dma((G_PIECES,)), dma((G_PIECES,)),
            dma((chunks,)), dma((chunks,)), dma, dma((4,)),
            dma((2,)), dma((2,)), dma((22,)), dma((22,)), dma((3,)), dma((3,)),
        ],
        compiler_params=pltpu.CompilerParams(collective_id=0, has_side_effects=True, vmem_limit_bytes=60 << 20),
        cost_estimate=pl.CostEstimate(flops=9 * 10**9, bytes_accessed=6 * 10**6, transcendentals=0),
        name="layer",
    )(*weights, *cotangents, tokens, gain, down, *ups)


def shards(
    tokens,
    gain,
    query_projection_weight,
    key_projection_weight,
    value_projection_weight,
    adapter_down_factors,
    query_adapter_up,
    key_adapter_up,
    value_adapter_up,
    query_cotangent,
    key_cotangent,
    value_cotangent,
):
    kinds, rank, full_width = adapter_down_factors.shape
    grad_tokens, grad_down, *grad_ups = layer(
        (query_projection_weight, key_projection_weight, value_projection_weight),
        (query_cotangent, key_cotangent, value_cotangent),
        tokens,
        gain.reshape(1, full_width),
        adapter_down_factors.reshape(kinds * rank, full_width),
        (query_adapter_up, key_adapter_up, value_adapter_up),
    )
    return (grad_tokens, grad_down.reshape(kinds, rank, -1), *grad_ups)


def solution(mesh):
    in_specs = (
        P("fsdp", "tp"),
        P(),
        P("fsdp", "tp"),
        P("fsdp", "tp"),
        P("fsdp", "tp"),
        P(),
        P(None, "tp"),
        P(None, "tp"),
        P(None, "tp"),
        P("fsdp", "tp"),
        P("fsdp", "tp"),
        P("fsdp", "tp"),
    )
    out_specs = (P("fsdp", "tp"), P(None, None, "tp"), P(None, "tp"), P(None, "tp"), P(None, "tp"))
    return jax.shard_map(shards, mesh=mesh, in_specs=in_specs, out_specs=out_specs, check_vma=False)
```

```python
import functools
import heapq
import math

import jax
import jax.numpy as jnp
from jax import lax
from jax.experimental import pallas as pl
from jax.experimental.pallas import tpu as pltpu
from jax.sharding import PartitionSpec as P

norm_eps = 1e-05
adapter_scale = 2.0

MESH = pl.DeviceIdType.MESH
NY, NZ = 4, 8
SLOT = 48
CHUNKS = (8, 8, 8, 8, 8, 8, 8, 6, 2)
G_PIECES = 8
G_TIME = 44.0
AR_USED = 25
OUT_PIECES = 4
VMEM_LIMIT = 60 << 20
MOVED = {(1, 2): ("y+", 0), (-1, -2): ("y-", 0)}


def forwards(have, item):
    part, dy, dz, half = item
    out = []
    if part == 0:
        if dz == 0:
            if dy == 0:
                out += [("y+", (0, 1, 0, None)), ("y-", (0, -1, 0, None))]
            elif dy == 1:
                out += [("y+", (0, 2, 0, 0))]
            elif dy == -1:
                out += [("y-", (0, 2, 0, 1))]
            if half is None or (0, 2, 0, 1 - half) in have:
                out += [("z+", (0, dy, 1, None)), ("z-", (0, dy, -1, None))]
        elif dz > 0:
            if (dy, dz + 1) not in MOVED and (dz < 3 or (dz == 3 and dy in (0, 1))):
                out += [("z+", (0, dy, dz + 1, None))]
        elif dz > -3:
            if (dy, dz - 1) not in MOVED:
                out += [("z-", (0, dy, dz - 1, None))]
        elif dy in (-1, 2):
            out += [("z-", (0, dy, 4, None))]
        out += [(link, (0, my, mz, None)) for (my, mz), (link, at) in MOVED.items() if (at, mz) == (dy, dz)]
    elif dy == 0:
        if dz == 0:
            out += [("z+", (1, 0, 1, None)), ("z-", (1, 0, -1, None))]
        elif 0 < dz < 4:
            out += [("z+", (1, 0, dz + 1, 0 if dz == 3 else None))]
        elif dz < 0:
            out += [("z-", (1, 0, 4 if dz == -3 else dz - 1, 1 if dz == -3 else None))]
        if half is None or (1, 0, 4, 1 - half) in have:
            out += [("y+", (1, 1, dz, None)), ("y-", (1, -1, dz, None))]
    elif dy == 1 and dz in (0, 1, 2, 3):
        out += [("y+", (1, 2, dz, None))]
    elif dy == -1 and dz in (-1, -2, -3, 4):
        out += [("y-", (1, 2, dz, None))]
    return out


def make_plan(rows, tasks, rate=44.0, latency=1.9, per_slot=0.23, per_half=0.15):
    size = [r * 4.096 for r in rows]
    starts = [sum(CHUNKS[:k]) for k in range(len(CHUNKS))]
    free = dict.fromkeys(("y+", "y-", "z+", "z-"), 0.0)
    have, events, actions, serial = set(), [], [], iter(range(1000))

    def issue(now, link, item):
        span = size[item[0]] * (1.0 if item[3] is None else 0.5) / rate
        free[link] = max(now, free[link]) + span
        heapq.heappush(events, (free[link] + latency, next(serial), item))

    first = []
    for item in ((0, 0, 0, None), (1, 0, 0, None)):
        have.add(item)
        first += forwards(have, item)
    first = [e for e in first if e[0][0] == "y"] + [e for e in reversed(first) if e[0][0] == "z"]
    for link, item in first:
        issue(0.0, link, item)
    slots = {(0, 0, 0): 0, (1, 0, 0): 1}
    tasks, now, done, owed, waiting = list(tasks), 0.0, 0, [], []
    ready = 0.0
    while events or tasks or done < len(CHUNKS) or owed or waiting:
        if events and events[0][0] <= now:
            item = heapq.heappop(events)[2]
            have.add(item)
            onward = forwards(have, item)
            now += 0.06
            for link, new in onward:
                issue(now, link, new)
            if item[3] is None or (*item[:3], 1 - item[3]) in have:
                slots[item[:3]] = len(slots)
            actions.append(("event", item, onward))
        elif tasks and ready <= now and (tasks[0][0] != "spread_z" or not events):
            name, span, axis, load, wait = tasks.pop(0)
            actions.append(("task", name, None))
            now += span
            ready = now
            for link in (axis + "+", axis + "-") if axis else ():
                free[link] = max(now, free[link]) + load
                ready = max(ready, free[link])
            ready += wait
        elif now >= G_TIME and owed:
            k = owed.pop(0)
            actions.append(("multiply", k, "mate"))
            now += per_half * CHUNKS[k]
            waiting.append((k, "mate"))
            if len(waiting) > 1:
                actions.append(("pass", *waiting.pop(0)))
                now += 0.1
        elif done < len(CHUNKS) and starts[done] + CHUNKS[done] <= len(slots):
            kind = "both" if now >= G_TIME - 2.0 else "own"
            actions.append(("multiply", done, kind))
            if kind == "own":
                owed.append(done)
            now += (per_half if kind == "own" else per_slot) * CHUNKS[done]
            waiting.append((done, kind))
            done += 1
            if len(waiting) > 1:
                actions.append(("pass", *waiting.pop(0)))
                now += 0.2
        elif waiting and (done == len(CHUNKS) or now < G_TIME):
            actions.append(("pass", *waiting.pop(0)))
            now += 0.2
        else:
            wake = [e[0] for e in events[:1]] + [ready] * (ready > now)
            now = max(now, min(wake + ([G_TIME] if now < G_TIME else [])))
    return first, actions, slots


TASKS = (
    ("low_products", 2.2, "", 0.0, 1.9),
    ("low_pair", 0.1, "", 0.0, 5.9),
    ("low_part", 0.1, "", 0.0, 1.6),
    ("low_all", 0.8, "", 0.0, 0.5),
    ("columns_ready", 0.6, "", 0.0, 0.5),
    ("adapter_term", 0.7, "", 0.0, 6.5),
    ("sum_x", 0.1, "y", 3.0, 4.0),
    ("sum_y", 0.1, "z", 1.5, 4.5),
    ("sum_z", 0.1, "", 0.0, 6.5),
    ("spread_x", 0.1, "z", 3.0, 4.5),
    ("spread_z", 0.1, "", 0.0, 0.0),
)


def dot_nt(a, b):
    return lax.dot_general(a, b, (((1,), (1,)), ((), ())), preferred_element_type=jnp.float32)


def as_column(row):
    return jnp.transpose(jnp.broadcast_to(row, (128, row.shape[1])))[:, :1]


def layer_kernel(
    rows, wq, wk, wv, gq, gk, gv, tokens_hbm, gain_all, down_all, uq, uk, uv,
    grad_out, adapter_out,
    wbuf, gbuf, keep, csend, crecv, xs, xr,
    tok, tok_t, acc, turned, grad_buf, gain_column, low, low_total, out_low_buf, inverse, inner_buf,
    arw, ar1, ar2, ar3, arg,
    load_sem, wsend_sem, wrecv_sem, gsend_sem, grecv_sem, csend_sem, crecv_sem, xsend_sem, xrecv_sem,
    lsend_sem, lrecv_sem, asend_sem, arecv_sem, isend_sem, irecv_sem, store_sem,
):
    f = lax.axis_index("fsdp")
    t = lax.axis_index("tp")
    y, z, x_lo = f // 16, (f // 2) % 8, f % 2
    x_hi, core = t // 2, t % 2
    tokens, owned_width = tokens_hbm.shape
    full_width = down_all.shape[1]
    f32, bf16 = jnp.float32, jnp.bfloat16
    first, actions, slots = make_plan(rows, TASKS)
    log = [(item, onward) for kind, item, onward in actions if kind == "event"]
    where = {v: k for k, v in slots.items()}

    def place(yy, zz, xx):
        return (yy % NY) * 16 + (zz % NZ) * 2 + xx

    link_device = {
        "y+": (place(y + 1, z, x_lo), t),
        "y-": (place(y + NY - 1, z, x_lo), t),
        "z+": (place(y, z + 1, x_lo), t),
        "z-": (place(y, z + NZ - 1, x_lo), t),
    }
    mate = (place(y, z, 1 - x_lo), t)
    twin = (f, x_hi * 2 + 1 - core)
    across = (f, (1 - x_hi) * 2 + core)

    def remote(src, dst, send_sem, recv_sem, device):
        return pltpu.make_async_remote_copy(
            src_ref=src, dst_ref=dst, send_sem=send_sem, recv_sem=recv_sem, device_id=device, device_id_type=MESH
        )

    def landed(ref, sem):
        pltpu.make_async_copy(ref, ref, sem).wait()

    started = []

    def send_now(*args):
        copy = remote(*args)
        copy.start()
        started.append(copy)
        return copy

    loads, token_load = [], pltpu.make_async_copy(tokens_hbm, tok, load_sem.at[9])
    own_half = (x_lo + core) % 2
    own_begin = pl.multiple_of(own_half * tokens, 128)
    column, spans = 0, []
    for index, (w, g) in enumerate(((wq, gq), (wk, gk), (wv, gv))):
        width = w.shape[1]
        columns = pl.ds(column, width)
        spans.append((column, width))
        loads.append(pltpu.make_async_copy(w.at[pl.ds(0, rows[0])], wbuf.at[0, pl.ds(0, rows[0]), columns], load_sem.at[3 * index]))
        loads.append(pltpu.make_async_copy(w.at[pl.ds(rows[0], rows[1])], wbuf.at[1, pl.ds(0, rows[1]), columns], load_sem.at[3 * index + 1]))
        column += width
    for index, g in enumerate((gq, gk, gv)):
        columns = pl.ds(*spans[index])
        loads.append(pltpu.make_async_copy(g, gbuf.at[pl.ds(own_begin, tokens), columns], load_sem.at[3 * index + 2]))
    for load in loads:
        load.start()
    token_load.start()

    barrier = pltpu.get_barrier_semaphore()
    partners = [(place(y + k, z, x_lo), t) for k in range(1, NY)] + [(place(y, z + k, x_lo), t) for k in range(1, NZ)]
    for dhi in (0, 1):
        for dlo in (0, 1):
            for dc in (0, 1):
                if dhi or dlo or dc:
                    partners.append((place(y, z, (x_lo + dlo) % 2), ((x_hi + dhi) % 2) * 2 + (core + dc) % 2))
    for device in partners:
        pl.semaphore_signal(barrier, inc=1, device_id=device, device_id_type=MESH)
    pl.semaphore_wait(barrier, len(partners))
    for load in loads:
        load.wait()

    event_index = {item: index for index, (item, _) in enumerate(log)}
    half_width = wbuf.shape[2] // 2

    def block(slot, part, half):
        if half is None:
            return wbuf.at[slot, pl.ds(0, rows[part])]
        return wbuf.at[slot, pl.ds(0, rows[part]), pl.ds(half * half_width, half_width)]

    def forward(origin, link, item):
        part, half, index = item[0], item[3], event_index[item]
        send_now(
            block(slots[origin[:3]], part, half), block(slots[item[:3]], part, half),
            wsend_sem.at[index], wrecv_sem.at[index], link_device[link],
        )

    for link, item in first:
        forward((item[0], 0, 0), link, item)

    g_lines = tokens // G_PIECES

    def g_piece(k):
        return gbuf.at[pl.ds(pl.multiple_of(own_half * tokens + k * g_lines, 16), g_lines)]

    def g_send(k):
        send_now(g_piece(k), g_piece(k), gsend_sem.at[k], grecv_sem.at[k], mate)

    def g_wait():
        for k in range(G_PIECES):
            landed(gbuf.at[pl.ds(0, g_lines)], grecv_sem.at[k])

    gain_lines = gain_all[pl.ds(t * (owned_width // 128), owned_width // 128)]
    gain_row = jnp.concatenate([gain_lines[k : k + 1] for k in range(owned_width // 128)], axis=1)
    down = down_all[:, pl.ds(pl.multiple_of(t * owned_width, 128), owned_width)]
    rank3, rank = down.shape[0], down.shape[0] // 3

    def low_products():
        token_load.wait()
        scaled = down.astype(f32) * gain_row
        high = scaled.astype(bf16)
        rest = scaled - high.astype(f32)
        middle = rest.astype(bf16)
        lowest = (rest - middle.astype(f32)).astype(bf16)
        lines = tok[...]
        for begin, part in ((0, high), (1, middle), (2, lowest)):
            term = dot_nt(part, lines)
            low[0, 0:rank3] = term if begin == 0 else low[0, 0:rank3] + term
        for m, up in enumerate((uq, uk, uv)):
            begin, width = spans[m]
            own = gbuf[pl.ds(own_begin, tokens), begin : begin + width]
            low[0, rank3 + m * rank : rank3 + (m + 1) * rank] = dot_nt(up[...], own)
        squares = lines.astype(f32) * lines.astype(f32)
        high = squares.astype(bf16)
        lowest = (squares - high.astype(f32)).astype(bf16)
        ones = jnp.ones((16, owned_width), bf16)
        low[0, 2 * rank3 :] = dot_nt(ones, high) + dot_nt(ones, lowest)
        send_now(low.at[0], low.at[1], lsend_sem.at[0], lrecv_sem.at[0], twin)

    my_part = pl.ds(pl.multiple_of(core * (low_total.shape[0] // 2), 8), low_total.shape[0] // 2)

    def low_pair():
        landed(low.at[1], lrecv_sem.at[0])
        low[2] = low[0] + low[1]
        send_now(low.at[2, my_part], low.at[3, my_part], lsend_sem.at[1], lrecv_sem.at[1], across)

    def low_part():
        landed(low.at[3, my_part], lrecv_sem.at[1])
        low_total[my_part] = low[2, my_part] + low[3, my_part]
        send_now(low_total.at[my_part], low_total.at[my_part], lsend_sem.at[2], lrecv_sem.at[2], twin)

    gradient_scale = adapter_scale / math.sqrt(tokens * 64)

    used = AR_USED

    class Lines:
        at = 0

    def pack(lines):
        for k in range(lines.shape[0] // 16):
            arw[Lines.at // 2, Lines.at % 2] = lines[k * 16 : (k + 1) * 16]
            Lines.at += 1

    def low_all():
        landed(low_total.at[my_part], lrecv_sem.at[2])
        inverse_row = lax.rsqrt(low_total[2 * rank3 : 2 * rank3 + 8] / full_width + norm_eps)
        inverse[...] = inverse_row
        in_low = (low_total[0:rank3] * inverse_row[:1]).astype(bf16)
        out_low = low_total[rank3 : 2 * rank3].astype(bf16)
        out_low_buf[...] = out_low
        unit = tok[...].astype(f32) * as_column(inverse_row[:1])
        normed = (unit * gain_row).astype(bf16)
        local = gradient_scale * jnp.dot(out_low, normed, preferred_element_type=f32)
        for j in range(owned_width // 128):
            pack(local[:, j * 128 : (j + 1) * 128])
        for m in range(3):
            begin, width = spans[m]
            own = gbuf[pl.ds(own_begin, tokens), begin : begin + width]
            local = gradient_scale * jnp.dot(in_low[m * rank : (m + 1) * rank], own, preferred_element_type=f32)
            for j in range(width // 128):
                pack(local[:, j * 128 : (j + 1) * 128])
        while Lines.at < 64:
            pack(jnp.zeros((16, 128), f32))
        send_now(arw.at[pl.ds(0, used), 1 - x_lo], ar1, asend_sem.at[0], arecv_sem.at[0], mate)

    def of_y(yy):
        return pl.ds(yy * NZ, NZ)

    def sum_x():
        landed(ar1, arecv_sem.at[0])
        arw[0:used, x_lo] = arw[0:used, x_lo] + ar1[...]
        for k in range(1, NY):
            other = (y + k) % NY
            send_now(arw.at[of_y(other), x_lo], ar2.at[k - 1], asend_sem.at[k], arecv_sem.at[k], (place(other, z, x_lo), t))

    def sum_y():
        for k in range(1, NY):
            landed(ar2.at[k - 1], arecv_sem.at[k])
        arw[of_y(y), x_lo] = arw[of_y(y), x_lo] + ar2[0] + ar2[1] + ar2[2]
        for k in range(1, NZ):
            other = (z + k) % NZ
            send_now(arw.at[y * NZ + other, x_lo], ar3.at[k - 1], asend_sem.at[3 + k], arecv_sem.at[3 + k], (place(y, other, x_lo), t))

    def sum_z():
        for k in range(1, NZ):
            landed(ar3.at[k - 1], arecv_sem.at[3 + k])
        total = arw[y * NZ + z, x_lo]
        for k in range(NZ - 1):
            total = total + ar3[k]
        arg[y * NZ + z, x_lo] = total
        mine = arg.at[y * NZ + z, x_lo]
        send_now(mine, mine, asend_sem.at[21], arecv_sem.at[21], mate)

    def spread_x():
        landed(ar3.at[0], arecv_sem.at[21])
        for k in range(1, NZ):
            mine = arg.at[y * NZ + z]
            send_now(mine, mine, asend_sem.at[10 + k], arecv_sem.at[10 + k], (place(y, z + k, x_lo), t))

    def spread_z():
        for k in range(1, NZ):
            landed(arg.at[0], arecv_sem.at[10 + k])
        for k in range(1, NY):
            mine = arg.at[of_y(y)]
            send_now(mine, mine, asend_sem.at[17 + k], arecv_sem.at[17 + k], (place(y + k, z, x_lo), t))

    def spread_y():
        for k in range(1, NY):
            landed(arg.at[pl.ds(0, NZ)], arecv_sem.at[17 + k])

    def columns_ready():
        gain_column[...] = jnp.transpose(jnp.broadcast_to(gain_row, (128, owned_width)))
        for j in range(owned_width // 128):
            tok_t[j * 128 : (j + 1) * 128] = jnp.transpose(tok[:, j * 128 : (j + 1) * 128].astype(f32))

    def adapter_term():
        acc[...] = adapter_scale * lax.dot_general(
            jnp.transpose(down.astype(f32)).astype(bf16), out_low_buf[...], (((1,), (0,)), ((), ())), preferred_element_type=f32
        )

    starts = [sum(CHUNKS[:k]) for k in range(len(CHUNKS))]
    same = x_lo == core
    my_chip = x_hi * 2 + x_lo

    def lines_of(k):
        return wbuf[starts[k] : starts[k] + CHUNKS[k]].reshape(CHUNKS[k] * SLOT, wbuf.shape[2])

    def hold(k, product):
        keep[starts[k] * SLOT : (starts[k] + CHUNKS[k]) * SLOT, :] = product

    def to_twin(k, product):
        both = pl.ds(starts[k], CHUNKS[k])
        csend[starts[k] : starts[k] + CHUNKS[k]] = product.astype(bf16).reshape(CHUNKS[k], SLOT, tokens)
        return remote(csend.at[both], crecv.at[both], csend_sem.at[k], crecv_sem.at[k], twin)

    def keeps(kind):
        return same if kind == "own" else jnp.logical_not(same)

    def multiply(k, kind):
        if kind == "both":
            product = dot_nt(lines_of(k), gbuf[...])
            hold(k, product[:, :tokens])
            to_twin(k, product[:, tokens:]).start()
            return
        half = own_half if kind == "own" else 1 - own_half
        product = dot_nt(lines_of(k), gbuf[pl.ds(pl.multiple_of(half * tokens, 128), tokens)])

        @pl.when(keeps(kind))
        def _():
            hold(k, product)

        @pl.when(jnp.logical_not(keeps(kind)))
        def _():
            to_twin(k, product).start()

    def pass_on(k, kind):
        if kind == "both":
            pass_lines(k)
        else:
            pl.when(keeps(kind))(functools.partial(pass_lines, k))

    def pass_lines(k):
        begin, count = starts[k], CHUNKS[k]
        landed(crecv.at[pl.ds(begin, count)], crecv_sem.at[k])
        got = crecv[begin : begin + count].reshape(count * SLOT, tokens).astype(f32)
        total = keep[begin * SLOT : (begin + count) * SLOT, :] + got
        xs[begin : begin + count] = total.astype(bf16).reshape(count, SLOT, tokens)
        for slot in range(begin, begin + count):
            part, dy, dz = where[slot]
            owner_y, owner_z = (y + NY - dy) % NY, (z + NZ - dz) % NZ
            src = xs.at[slot, pl.ds(0, rows[part])]
            dst = xr.at[my_chip, owner_z, pl.ds(part * rows[0], rows[part])]
            own = jnp.logical_and(same, owner_y == t)

            @pl.when(own)
            def _():
                pltpu.make_async_copy(src, dst, xrecv_sem.at[my_chip]).start()

            @pl.when(jnp.logical_not(own))
            def _():
                remote(src, dst, xsend_sem, xrecv_sem.at[my_chip], (place(y, z, core), owner_y)).start()

    g_send(0)
    tasks = {
        "low_products": (low_products,),
        "low_pair": (low_pair, functools.partial(g_send, 1), functools.partial(g_send, 2)),
        "low_part": (low_part,),
        "low_all": (low_all, *(functools.partial(g_send, k) for k in range(3, G_PIECES))),
        "columns_ready": (columns_ready,),
        "adapter_term": (adapter_term,),
        "sum_x": (sum_x,),
        "sum_y": (sum_y,),
        "sum_z": (sum_z,),
        "spread_x": (spread_x,),
        "spread_z": (spread_z,),
    }
    g_here = False
    for kind, what, onward in actions:
        if kind == "event":
            landed(block(slots[what[:3]], what[0], what[3]), wrecv_sem.at[event_index[what]])
            for link, new in onward:
                forward(what, link, new)
        elif kind == "task":
            for task in tasks[what]:
                task()
        elif kind == "multiply":
            if onward != "own" and not g_here:
                g_wait()
                g_here = True
            multiply(what, onward)
        else:
            pass_on(what, onward)
    for chip in range(4):
        landed(xr.at[chip], xrecv_sem.at[chip])

    inverse_row = inverse[:1]
    inner = jnp.zeros((8, tokens), f32)
    for owner_z in range(NZ):
        for half in range(2):
            begin = (owner_z * 2 + half) * (rows[0] + rows[1])
            lines = pl.ds(begin, rows[0] + rows[1])
            back = xr[half, owner_z].astype(f32) + xr[2 + half, owner_z].astype(f32) + acc[lines]
            gained = gain_column[lines, :1] * back
            acc[lines] = gained
            product = gained * (tok_t[lines] * inverse_row)
            inner = inner + product.reshape(-1, 8, tokens).sum(axis=0)
    inner_buf[0] = inner
    for k, device in enumerate((twin, across, (f, (1 - x_hi) * 2 + 1 - core))):
        send_now(inner_buf.at[0], inner_buf.at[k + 1], isend_sem.at[k], irecv_sem.at[k], device)
    for j in range(owned_width // 128):
        turned[:, j * 128 : (j + 1) * 128] = jnp.transpose(acc[j * 128 : (j + 1) * 128])
    inverse_column = as_column(inverse_row)
    spread_y()
    stores = [pltpu.make_async_copy(arg.at[pl.ds(0, used)], adapter_out, store_sem.at[0])]
    stores[0].start()
    for k in range(3):
        landed(inner_buf.at[k + 1], irecv_sem.at[k])
    total = (inner_buf[0] + inner_buf[1]) + (inner_buf[2] + inner_buf[3])
    inner_column = as_column(jnp.sum(total, axis=0, keepdims=True) / full_width)
    step = tokens // OUT_PIECES
    for k in range(OUT_PIECES):
        lines = slice(k * step, (k + 1) * step)
        scale = inverse_column[lines]
        unit = tok[lines].astype(f32) * scale
        grad_buf[lines] = (scale * (turned[lines] - unit * inner_column[lines])).astype(bf16)
        stores.append(pltpu.make_async_copy(grad_buf.at[pl.ds(k * step, step)], grad_out.at[pl.ds(k * step, step)], store_sem.at[1 + k]))
        stores[-1].start()
    for copy in started:
        copy.wait_send()
    for k in range(len(CHUNKS)):
        both = pl.ds(starts[k], CHUNKS[k])
        landed(csend.at[both], csend_sem.at[k])
    @pl.when(same)
    def _():
        landed(xr.at[pl.ds(0, 3)], xsend_sem)

    @pl.when(jnp.logical_not(same))
    def _():
        landed(xr, xsend_sem)

    for copy in stores:
        copy.wait()


def layer(weights, cotangents, tokens, gain, down, ups):
    count, owned_width = tokens.shape
    owned = weights[0].shape[0]
    rows = (40, owned - 40)
    width = sum(w.shape[1] for w in weights)
    events = sum(kind == "event" for kind, _, _ in make_plan(rows, TASKS)[1])
    slots = 2 * NY * NZ
    chunks = len(CHUNKS)
    rank3 = down.shape[0]
    f32, bf16, dma = jnp.float32, jnp.bfloat16, pltpu.SemaphoreType.DMA
    vmem = pl.BlockSpec(memory_space=pltpu.VMEM)
    return pl.pallas_call(
        functools.partial(layer_kernel, rows),
        out_shape=(
            jax.ShapeDtypeStruct((count, owned_width), bf16),
            jax.ShapeDtypeStruct((AR_USED, 2, 16, 128), f32),
        ),
        in_specs=[pl.BlockSpec(memory_space=pl.ANY)] * 7 + [vmem] * 5,
        out_specs=(pl.BlockSpec(memory_space=pl.ANY),) * 2,
        scratch_shapes=[
            pltpu.VMEM((slots, SLOT, width), bf16),
            pltpu.VMEM((2 * count, width), bf16),
            pltpu.VMEM((slots * SLOT, count), f32),
            pltpu.VMEM((slots, SLOT, count), bf16),
            pltpu.VMEM((slots, SLOT, count), bf16),
            pltpu.VMEM((slots, SLOT, count), bf16),
            pltpu.VMEM((4, NZ, owned, count), bf16),
            pltpu.VMEM((count, owned_width), bf16),
            pltpu.VMEM((owned_width, count), f32),
            pltpu.VMEM((owned_width, count), f32),
            pltpu.VMEM((count, owned_width), f32),
            pltpu.VMEM((count, owned_width), bf16),
            pltpu.VMEM((owned_width, 128), f32),
            pltpu.VMEM((4, 2 * rank3 + 16, count), f32),
            pltpu.VMEM((2 * rank3 + 16, count), f32),
            pltpu.VMEM((rank3, count), bf16),
            pltpu.VMEM((8, count), f32),
            pltpu.VMEM((4, 8, count), f32),
            pltpu.VMEM((NY * NZ, 2, 16, 128), f32),
            pltpu.VMEM((AR_USED, 16, 128), f32),
            pltpu.VMEM((NY - 1, NZ, 16, 128), f32),
            pltpu.VMEM((NZ - 1, 16, 128), f32),
            pltpu.VMEM((NY * NZ, 2, 16, 128), f32),
            dma((10,)), dma((events,)), dma((events,)), dma((G_PIECES,)), dma((G_PIECES,)),
            dma((chunks,)), dma((chunks,)), dma, dma((4,)),
            dma((3,)), dma((3,)), dma((22,)), dma((22,)), dma((3,)), dma((3,)), dma((1 + OUT_PIECES,)),
        ],
        compiler_params=pltpu.CompilerParams(collective_id=0, has_side_effects=True, vmem_limit_bytes=VMEM_LIMIT),
        cost_estimate=pl.CostEstimate(flops=9 * 10**9, bytes_accessed=6 * 10**6, transcendentals=0),
        name="layer",
    )(*weights, *cotangents, tokens, gain, down, *ups)


def finish_kernel(grad_in, adapter, grad, down, upq, upk, upv):
    @pl.when(pl.program_id(0) == 0)
    def _():
        at = 0
        for ref in (down, upq, upk, upv):
            for j in range(ref.shape[1] // 128):
                for k in range(ref.shape[0] // 16):
                    ref[k * 16 : (k + 1) * 16, j * 128 : (j + 1) * 128] = adapter[at // 2, at % 2]
                    at += 1

    grad[...] = grad_in[...]


def finish(grad, adapter, rank3, ups):
    count, owned_width = grad.shape
    steps = 4
    f32 = jnp.float32
    shapes = [(rank3, owned_width)] + [u.shape for u in ups]
    block = pl.BlockSpec((count // steps, owned_width), lambda i: (i, 0))
    return pl.pallas_call(
        finish_kernel,
        grid=(steps,),
        out_shape=(jax.ShapeDtypeStruct(grad.shape, grad.dtype), *(jax.ShapeDtypeStruct(s, f32) for s in shapes)),
        in_specs=[block, pl.BlockSpec(adapter.shape, lambda i: (0, 0, 0, 0))],
        out_specs=(block, *(pl.BlockSpec(s, lambda i: (0, 0)) for s in shapes)),
        name="finish",
    )(grad, adapter)


def shards(
    tokens,
    gain,
    query_projection_weight,
    key_projection_weight,
    value_projection_weight,
    adapter_down_factors,
    query_adapter_up,
    key_adapter_up,
    value_adapter_up,
    query_cotangent,
    key_cotangent,
    value_cotangent,
):
    kinds, rank, full_width = adapter_down_factors.shape
    ups = (query_adapter_up, key_adapter_up, value_adapter_up)
    grad_tokens, adapter = layer(
        (query_projection_weight, key_projection_weight, value_projection_weight),
        (query_cotangent, key_cotangent, value_cotangent),
        tokens,
        gain.reshape(-1, 128),
        adapter_down_factors.reshape(kinds * rank, full_width),
        ups,
    )
    grad_tokens, grad_down, *grad_ups = finish(grad_tokens, adapter, kinds * rank, ups)
    return (grad_tokens, grad_down.reshape(kinds, rank, -1), *grad_ups)


def solution(mesh):
    in_specs = (
        P("fsdp", "tp"),
        P(),
        P("fsdp", "tp"),
        P("fsdp", "tp"),
        P("fsdp", "tp"),
        P(),
        P(None, "tp"),
        P(None, "tp"),
        P(None, "tp"),
        P("fsdp", "tp"),
        P("fsdp", "tp"),
        P("fsdp", "tp"),
    )
    out_specs = (P("fsdp", "tp"), P(None, None, "tp"), P(None, "tp"), P(None, "tp"), P(None, "tp"))
    return jax.shard_map(shards, mesh=mesh, in_specs=in_specs, out_specs=out_specs, check_vma=False)
```

```python
import functools
import heapq
import math

import jax
import jax.numpy as jnp
from jax import lax
from jax.experimental import pallas as pl
from jax.experimental.pallas import tpu as pltpu
from jax.sharding import PartitionSpec as P

norm_eps = 1e-05
adapter_scale = 2.0

MESH = pl.DeviceIdType.MESH
NY, NZ = 4, 8
SLOT = 48
CHUNKS = (8, 8, 8, 8, 8, 8, 4, 4, 3, 3, 2)
G_PIECES = 8
G_TIME = 44.0
LAST = ("spread_x", "spread_z")
AR_USED = 25
OUT_PIECES = 4
VMEM_LIMIT = 50 << 20
MOVED = {(1, 2): ("y+", 0), (-1, -2): ("y-", 0)}


def forwards(have, item):
    part, dy, dz, half = item
    out = []
    if part == 0:
        if dz == 0:
            if dy == 0:
                out += [("y+", (0, 1, 0, None)), ("y-", (0, -1, 0, None))]
            elif dy == 1:
                out += [("y+", (0, 2, 0, 0))]
            elif dy == -1:
                out += [("y-", (0, 2, 0, 1))]
            if half is None or (0, 2, 0, 1 - half) in have:
                out += [("z+", (0, dy, 1, None)), ("z-", (0, dy, -1, None))]
        elif dz > 0:
            if (dy, dz + 1) not in MOVED and (dz < 3 or (dz == 3 and dy in (0, 1))):
                out += [("z+", (0, dy, dz + 1, None))]
        elif dz > -3:
            if (dy, dz - 1) not in MOVED:
                out += [("z-", (0, dy, dz - 1, None))]
        elif dy in (-1, 2):
            out += [("z-", (0, dy, 4, None))]
        out += [(link, (0, my, mz, None)) for (my, mz), (link, at) in MOVED.items() if (at, mz) == (dy, dz)]
    elif dy == 0:
        if dz == 0:
            out += [("z+", (1, 0, 1, None)), ("z-", (1, 0, -1, None))]
        elif 0 < dz < 4:
            out += [("z+", (1, 0, dz + 1, 0 if dz == 3 else None))]
        elif dz < 0:
            out += [("z-", (1, 0, 4 if dz == -3 else dz - 1, 1 if dz == -3 else None))]
        if half is None or (1, 0, 4, 1 - half) in have:
            out += [("y+", (1, 1, dz, None)), ("y-", (1, -1, dz, None))]
    elif dy == 1 and dz in (0, 1, 2, 3):
        out += [("y+", (1, 2, dz, None))]
    elif dy == -1 and dz in (-1, -2, -3, 4):
        out += [("y-", (1, 2, dz, None))]
    return out


def make_plan(rows, tasks, rate=44.0, latency=1.9, per_slot=0.23, per_half=0.13, twin=2.6):
    size = [r * 4.096 for r in rows]
    starts = [sum(CHUNKS[:k]) for k in range(len(CHUNKS))]
    free = dict.fromkeys(("y+", "y-", "z+", "z-"), 0.0)
    have, events, actions, serial = set(), [], [], iter(range(1000))

    def issue(now, link, item):
        span = size[item[0]] * (1.0 if item[3] is None else 0.5) / rate
        free[link] = max(now, free[link]) + span
        heapq.heappush(events, (free[link] + latency, next(serial), item))

    first = []
    for item in ((0, 0, 0, None), (1, 0, 0, None)):
        have.add(item)
        first += forwards(have, item)
    first = [e for e in first if e[0][0] == "y"] + [e for e in reversed(first) if e[0][0] == "z"]
    for link, item in first:
        issue(0.0, link, item)
    slots = {(0, 0, 0): 0, (1, 0, 0): 1}
    tasks, now, done, owed, waiting = list(tasks), 0.0, 0, [], []
    ready = 0.0
    while events or tasks or done < len(CHUNKS) or owed or waiting:
        if events and events[0][0] <= now:
            item = heapq.heappop(events)[2]
            have.add(item)
            onward = forwards(have, item)
            now += 0.06
            for link, new in onward:
                issue(now, link, new)
            if item[3] is None or (*item[:3], 1 - item[3]) in have:
                slots[item[:3]] = len(slots)
            actions.append(("event", item, onward))
        elif tasks and ready <= now and (tasks[0][0] not in LAST or not events):
            name, span, axis, load, wait = tasks.pop(0)
            actions.append(("task", name, None))
            now += span
            ready = now
            for link in (axis + "+", axis + "-") if axis else ():
                free[link] = max(now, free[link]) + load
                ready = max(ready, free[link])
            ready += wait
        elif waiting and waiting[0][0] <= now:
            actions.append(("pass", *waiting.pop(0)[1:]))
            now += 0.3
        elif now >= G_TIME and owed:
            k = owed.pop(0)
            actions.append(("multiply", k, "mate"))
            now += per_half * CHUNKS[k]
            waiting.append((now + twin, k, "mate"))
        elif done < len(CHUNKS) and starts[done] + CHUNKS[done] <= len(slots):
            kind = "both" if now >= G_TIME - 2.0 else "own"
            actions.append(("multiply", done, kind))
            if kind == "own":
                owed.append(done)
            now += (per_half if kind == "own" else per_slot) * CHUNKS[done]
            waiting.append((now + twin, done, kind))
            done += 1
        else:
            wake = [e[0] for e in events[:1]] + [e[0] for e in waiting[:1]] + [ready] * (ready > now)
            now = max(now, min(wake + ([G_TIME] if now < G_TIME else [])))
    return first, actions, slots


TASKS = (
    ("low_products", 2.2, "", 0.0, 1.9),
    ("low_pair", 0.1, "", 0.0, 5.9),
    ("low_part", 0.1, "", 0.0, 1.6),
    ("low_all", 0.8, "", 0.0, 0.5),
    ("columns_ready", 0.6, "", 0.0, 0.5),
    ("adapter_term", 0.7, "", 0.0, 6.5),
    ("sum_x", 0.1, "y", 3.0, 4.0),
    ("sum_y", 0.1, "z", 1.5, 4.5),
    ("sum_z", 0.1, "", 0.0, 6.5),
    ("spread_x", 0.1, "z", 3.0, 4.5),
    ("spread_z", 0.1, "", 0.0, 0.0),
)


def dot_nt(a, b):
    return lax.dot_general(a, b, (((1,), (1,)), ((), ())), preferred_element_type=jnp.float32)


def as_column(row):
    return jnp.transpose(jnp.broadcast_to(row, (128, row.shape[1])))[:, :1]


def layer_kernel(
    rows, wq, wk, wv, gq, gk, gv, tokens_hbm, gain_hbm, down_hbm, uq_hbm, uk_hbm, uv_hbm,
    grad_out, adapter_out,
    wbuf, gbuf, keep, csend, crecv, xs, xr,
    gain_all, down_all, uq, uk, uv, tok, tok_t, acc, turned, grad_buf, gain_column, low, low_total, out_low_buf, inverse, inner_buf,
    arw, ar1, ar2, ar3, arg,
    load_sem, wsend_sem, wrecv_sem, gsend_sem, grecv_sem, csend_sem, crecv_sem, xsend_sem, xrecv_sem,
    lsend_sem, lrecv_sem, asend_sem, arecv_sem, isend_sem, irecv_sem, store_sem,
):
    f = lax.axis_index("fsdp")
    t = lax.axis_index("tp")
    y, z, x_lo = f // 16, (f // 2) % 8, f % 2
    x_hi, core = t // 2, t % 2
    tokens, owned_width = tokens_hbm.shape
    full_width = down_all.shape[1]
    f32, bf16 = jnp.float32, jnp.bfloat16
    first, actions, slots = make_plan(rows, TASKS)
    log = [(item, onward) for kind, item, onward in actions if kind == "event"]
    where = {v: k for k, v in slots.items()}

    def place(yy, zz, xx):
        return (yy % NY) * 16 + (zz % NZ) * 2 + xx

    link_device = {
        "y+": (place(y + 1, z, x_lo), t),
        "y-": (place(y + NY - 1, z, x_lo), t),
        "z+": (place(y, z + 1, x_lo), t),
        "z-": (place(y, z + NZ - 1, x_lo), t),
    }
    mate = (place(y, z, 1 - x_lo), t)
    twin = (f, x_hi * 2 + 1 - core)
    across = (f, (1 - x_hi) * 2 + core)

    def remote(src, dst, send_sem, recv_sem, device):
        return pltpu.make_async_remote_copy(
            src_ref=src, dst_ref=dst, send_sem=send_sem, recv_sem=recv_sem, device_id=device, device_id_type=MESH
        )

    def landed(ref, sem):
        pltpu.make_async_copy(ref, ref, sem).wait()

    started = []

    def send_now(*args):
        copy = remote(*args)
        copy.start()
        started.append(copy)
        return copy

    loads, token_load = [], pltpu.make_async_copy(tokens_hbm, tok, load_sem.at[9])
    own_half = (x_lo + core) % 2
    own_begin = pl.multiple_of(own_half * tokens, 128)
    column, spans = 0, []
    for index, (w, g) in enumerate(((wq, gq), (wk, gk), (wv, gv))):
        width = w.shape[1]
        columns = pl.ds(column, width)
        spans.append((column, width))
        loads.append(pltpu.make_async_copy(w.at[pl.ds(0, rows[0])], wbuf.at[0, pl.ds(0, rows[0]), columns], load_sem.at[3 * index]))
        loads.append(pltpu.make_async_copy(w.at[pl.ds(rows[0], rows[1])], wbuf.at[1, pl.ds(0, rows[1]), columns], load_sem.at[3 * index + 1]))
        column += width
    for index, g in enumerate((gq, gk, gv)):
        columns = pl.ds(*spans[index])
        loads.append(pltpu.make_async_copy(g, gbuf.at[pl.ds(own_begin, tokens), columns], load_sem.at[3 * index + 2]))
    for load in loads:
        load.start()
    small = ((gain_hbm, gain_all), (down_hbm, down_all), (uq_hbm, uq), (uk_hbm, uk), (uv_hbm, uv))
    for index, (src, dst) in enumerate(small):
        loads.append(pltpu.make_async_copy(src, dst, load_sem.at[10 + index]))
        loads[-1].start()
    token_load.start()

    barrier = pltpu.get_barrier_semaphore()
    partners = [(place(y + k, z, x_lo), t) for k in range(1, NY)] + [(place(y, z + k, x_lo), t) for k in range(1, NZ)]
    for dhi in (0, 1):
        for dlo in (0, 1):
            for dc in (0, 1):
                if dhi or dlo or dc:
                    partners.append((place(y, z, (x_lo + dlo) % 2), ((x_hi + dhi) % 2) * 2 + (core + dc) % 2))
    for device in partners:
        pl.semaphore_signal(barrier, inc=1, device_id=device, device_id_type=MESH)
    pl.semaphore_wait(barrier, len(partners))
    for load in loads:
        load.wait()

    event_index = {item: index for index, (item, _) in enumerate(log)}
    half_width = wbuf.shape[2] // 2

    def block(slot, part, half):
        if half is None:
            return wbuf.at[slot, pl.ds(0, rows[part])]
        return wbuf.at[slot, pl.ds(0, rows[part]), pl.ds(half * half_width, half_width)]

    def forward(origin, link, item):
        part, half, index = item[0], item[3], event_index[item]
        send_now(
            block(slots[origin[:3]], part, half), block(slots[item[:3]], part, half),
            wsend_sem.at[index], wrecv_sem.at[index], link_device[link],
        )

    for link, item in first:
        forward((item[0], 0, 0), link, item)

    g_lines = tokens // G_PIECES

    def g_piece(k):
        return gbuf.at[pl.ds(pl.multiple_of(own_half * tokens + k * g_lines, 16), g_lines)]

    def g_send(k):
        send_now(g_piece(k), g_piece(k), gsend_sem.at[k], grecv_sem.at[k], mate)

    def g_wait():
        for k in range(G_PIECES):
            landed(gbuf.at[pl.ds(0, g_lines)], grecv_sem.at[k])

    gain_lines = gain_all[pl.ds(t * (owned_width // 128), owned_width // 128)]
    gain_row = jnp.concatenate([gain_lines[k : k + 1] for k in range(owned_width // 128)], axis=1)
    down = down_all[:, pl.ds(pl.multiple_of(t * owned_width, 128), owned_width)]
    rank3, rank = down.shape[0], down.shape[0] // 3

    def low_products():
        token_load.wait()
        scaled = down.astype(f32) * gain_row
        high = scaled.astype(bf16)
        rest = scaled - high.astype(f32)
        middle = rest.astype(bf16)
        lowest = (rest - middle.astype(f32)).astype(bf16)
        lines = tok[...]
        for begin, part in ((0, high), (1, middle), (2, lowest)):
            term = dot_nt(part, lines)
            low[0, 0:rank3] = term if begin == 0 else low[0, 0:rank3] + term
        for m, up in enumerate((uq, uk, uv)):
            begin, width = spans[m]
            own = gbuf[pl.ds(own_begin, tokens), begin : begin + width]
            low[0, rank3 + m * rank : rank3 + (m + 1) * rank] = dot_nt(up[...], own)
        squares = lines.astype(f32) * lines.astype(f32)
        high = squares.astype(bf16)
        lowest = (squares - high.astype(f32)).astype(bf16)
        ones = jnp.ones((16, owned_width), bf16)
        low[0, 2 * rank3 :] = dot_nt(ones, high) + dot_nt(ones, lowest)
        send_now(low.at[0], low.at[1], lsend_sem.at[0], lrecv_sem.at[0], twin)

    my_part = pl.ds(pl.multiple_of(core * (low_total.shape[0] // 2), 8), low_total.shape[0] // 2)

    def low_pair():
        landed(low.at[1], lrecv_sem.at[0])
        low[2] = low[0] + low[1]
        send_now(low.at[2, my_part], low.at[3, my_part], lsend_sem.at[1], lrecv_sem.at[1], across)

    def low_part():
        landed(low.at[3, my_part], lrecv_sem.at[1])
        low_total[my_part] = low[2, my_part] + low[3, my_part]
        send_now(low_total.at[my_part], low_total.at[my_part], lsend_sem.at[2], lrecv_sem.at[2], twin)

    gradient_scale = adapter_scale / math.sqrt(tokens * 64)

    used = AR_USED

    class Lines:
        at = 0

    def pack(lines):
        for k in range(lines.shape[0] // 16):
            arw[Lines.at // 2, Lines.at % 2] = lines[k * 16 : (k + 1) * 16]
            Lines.at += 1

    def low_all():
        landed(low_total.at[my_part], lrecv_sem.at[2])
        inverse_row = lax.rsqrt(low_total[2 * rank3 : 2 * rank3 + 8] / full_width + norm_eps)
        inverse[...] = inverse_row
        in_low = (low_total[0:rank3] * inverse_row[:1]).astype(bf16)
        out_low = low_total[rank3 : 2 * rank3].astype(bf16)
        out_low_buf[...] = out_low
        unit = tok[...].astype(f32) * as_column(inverse_row[:1])
        normed = (unit * gain_row).astype(bf16)
        local = gradient_scale * jnp.dot(out_low, normed, preferred_element_type=f32)
        for j in range(owned_width // 128):
            pack(local[:, j * 128 : (j + 1) * 128])
        for m in range(3):
            begin, width = spans[m]
            own = gbuf[pl.ds(own_begin, tokens), begin : begin + width]
            local = gradient_scale * jnp.dot(in_low[m * rank : (m + 1) * rank], own, preferred_element_type=f32)
            for j in range(width // 128):
                pack(local[:, j * 128 : (j + 1) * 128])
        while Lines.at < 64:
            pack(jnp.zeros((16, 128), f32))
        send_now(arw.at[pl.ds(0, used), 1 - x_lo], ar1, asend_sem.at[0], arecv_sem.at[0], mate)

    def of_y(yy):
        return pl.ds(yy * NZ, NZ)

    def sum_x():
        landed(ar1, arecv_sem.at[0])
        arw[0:used, x_lo] = arw[0:used, x_lo] + ar1[...]
        for k in range(1, NY):
            other = (y + k) % NY
            send_now(arw.at[of_y(other), x_lo], ar2.at[k - 1], asend_sem.at[k], arecv_sem.at[k], (place(other, z, x_lo), t))

    def sum_y():
        for k in range(1, NY):
            landed(ar2.at[k - 1], arecv_sem.at[k])
        arw[of_y(y), x_lo] = arw[of_y(y), x_lo] + ar2[0] + ar2[1] + ar2[2]
        for k in range(1, NZ):
            other = (z + k) % NZ
            send_now(arw.at[y * NZ + other, x_lo], ar3.at[k - 1], asend_sem.at[3 + k], arecv_sem.at[3 + k], (place(y, other, x_lo), t))

    def sum_z():
        for k in range(1, NZ):
            landed(ar3.at[k - 1], arecv_sem.at[3 + k])
        total = arw[y * NZ + z, x_lo]
        for k in range(NZ - 1):
            total = total + ar3[k]
        arg[y * NZ + z, x_lo] = total
        mine = arg.at[y * NZ + z, x_lo]
        send_now(mine, mine, asend_sem.at[21], arecv_sem.at[21], mate)

    def spread_x():
        landed(ar3.at[0], arecv_sem.at[21])
        for k in range(1, NZ):
            mine = arg.at[y * NZ + z]
            send_now(mine, mine, asend_sem.at[10 + k], arecv_sem.at[10 + k], (place(y, z + k, x_lo), t))

    def spread_z():
        for k in range(1, NZ):
            landed(arg.at[0], arecv_sem.at[10 + k])
        for k in range(1, NY):
            mine = arg.at[of_y(y)]
            send_now(mine, mine, asend_sem.at[17 + k], arecv_sem.at[17 + k], (place(y + k, z, x_lo), t))

    def spread_y():
        for k in range(1, NY):
            landed(arg.at[pl.ds(0, NZ)], arecv_sem.at[17 + k])

    def columns_ready():
        gain_column[...] = jnp.transpose(jnp.broadcast_to(gain_row, (128, owned_width)))
        for j in range(owned_width // 128):
            tok_t[j * 128 : (j + 1) * 128] = jnp.transpose(tok[:, j * 128 : (j + 1) * 128].astype(f32))

    def adapter_term():
        acc[...] = adapter_scale * lax.dot_general(
            jnp.transpose(down.astype(f32)).astype(bf16), out_low_buf[...], (((1,), (0,)), ((), ())), preferred_element_type=f32
        )

    starts = [sum(CHUNKS[:k]) for k in range(len(CHUNKS))]
    same = x_lo == core
    my_chip = x_hi * 2 + x_lo

    def lines_of(k):
        return wbuf[starts[k] : starts[k] + CHUNKS[k]].reshape(CHUNKS[k] * SLOT, wbuf.shape[2])

    def hold(k, product):
        keep[starts[k] * SLOT : (starts[k] + CHUNKS[k]) * SLOT, :] = product

    def to_twin(k, product):
        both = pl.ds(starts[k], CHUNKS[k])
        csend[starts[k] : starts[k] + CHUNKS[k]] = product.astype(bf16).reshape(CHUNKS[k], SLOT, tokens)
        return remote(csend.at[both], crecv.at[both], csend_sem.at[k], crecv_sem.at[k], twin)

    def keeps(kind):
        return same if kind == "own" else jnp.logical_not(same)

    def multiply(k, kind):
        if kind == "both":
            product = dot_nt(lines_of(k), gbuf[...])
            hold(k, product[:, :tokens])
            to_twin(k, product[:, tokens:]).start()
            return
        half = own_half if kind == "own" else 1 - own_half
        product = dot_nt(lines_of(k), gbuf[pl.ds(pl.multiple_of(half * tokens, 128), tokens)])

        @pl.when(keeps(kind))
        def _():
            hold(k, product)

        @pl.when(jnp.logical_not(keeps(kind)))
        def _():
            to_twin(k, product).start()

    def pass_on(k, kind):
        if kind == "both":
            pass_lines(k)
        else:
            pl.when(keeps(kind))(functools.partial(pass_lines, k))

    def pass_lines(k):
        begin, count = starts[k], CHUNKS[k]
        landed(crecv.at[pl.ds(begin, count)], crecv_sem.at[k])
        got = crecv[begin : begin + count].reshape(count * SLOT, tokens).astype(f32)
        total = keep[begin * SLOT : (begin + count) * SLOT, :] + got
        xs[begin : begin + count] = total.astype(bf16).reshape(count, SLOT, tokens)
        for slot in range(begin, begin + count):
            part, dy, dz = where[slot]
            owner_y, owner_z = (y + NY - dy) % NY, (z + NZ - dz) % NZ
            src = xs.at[slot, pl.ds(0, rows[part])]
            dst = xr.at[my_chip, owner_z, pl.ds(part * rows[0], rows[part])]
            own = jnp.logical_and(same, owner_y == t)

            @pl.when(own)
            def _():
                pltpu.make_async_copy(src, dst, xrecv_sem.at[my_chip]).start()

            @pl.when(jnp.logical_not(own))
            def _():
                remote(src, dst, xsend_sem, xrecv_sem.at[my_chip], (place(y, z, core), owner_y)).start()

    g_send(0)
    tasks = {
        "low_products": (low_products,),
        "low_pair": (low_pair, functools.partial(g_send, 1), functools.partial(g_send, 2)),
        "low_part": (low_part,),
        "low_all": (low_all, *(functools.partial(g_send, k) for k in range(3, G_PIECES))),
        "columns_ready": (columns_ready,),
        "adapter_term": (adapter_term,),
        "sum_x": (sum_x,),
        "sum_y": (sum_y,),
        "sum_z": (sum_z,),
        "spread_x": (spread_x,),
        "spread_z": (spread_z,),
    }
    g_here = False
    for kind, what, onward in actions:
        if kind == "event":
            landed(block(slots[what[:3]], what[0], what[3]), wrecv_sem.at[event_index[what]])
            for link, new in onward:
                forward(what, link, new)
        elif kind == "task":
            for task in tasks[what]:
                task()
        elif kind == "multiply":
            if onward != "own" and not g_here:
                g_wait()
                g_here = True
            multiply(what, onward)
        else:
            pass_on(what, onward)
    for chip in range(4):
        landed(xr.at[chip], xrecv_sem.at[chip])

    inverse_row = inverse[:1]
    inner = jnp.zeros((8, tokens), f32)
    for owner_z in range(NZ):
        for half in range(2):
            begin = (owner_z * 2 + half) * (rows[0] + rows[1])
            lines = pl.ds(begin, rows[0] + rows[1])
            back = xr[half, owner_z].astype(f32) + xr[2 + half, owner_z].astype(f32) + acc[lines]
            gained = gain_column[lines, :1] * back
            acc[lines] = gained
            product = gained * (tok_t[lines] * inverse_row)
            inner = inner + product.reshape(-1, 8, tokens).sum(axis=0)
    inner_buf[0] = inner
    for k, device in enumerate((twin, across, (f, (1 - x_hi) * 2 + 1 - core))):
        send_now(inner_buf.at[0], inner_buf.at[k + 1], isend_sem.at[k], irecv_sem.at[k], device)
    for j in range(owned_width // 128):
        turned[:, j * 128 : (j + 1) * 128] = jnp.transpose(acc[j * 128 : (j + 1) * 128])
    inverse_column = as_column(inverse_row)
    spread_y()
    stores = [pltpu.make_async_copy(arg.at[pl.ds(0, used)], adapter_out, store_sem.at[0])]
    stores[0].start()
    for k in range(3):
        landed(inner_buf.at[k + 1], irecv_sem.at[k])
    total = (inner_buf[0] + inner_buf[1]) + (inner_buf[2] + inner_buf[3])
    inner_column = as_column(jnp.sum(total, axis=0, keepdims=True) / full_width)
    step = tokens // OUT_PIECES
    for k in range(OUT_PIECES):
        lines = slice(k * step, (k + 1) * step)
        scale = inverse_column[lines]
        unit = tok[lines].astype(f32) * scale
        grad_buf[lines] = (scale * (turned[lines] - unit * inner_column[lines])).astype(bf16)
        stores.append(pltpu.make_async_copy(grad_buf.at[pl.ds(k * step, step)], grad_out.at[pl.ds(k * step, step)], store_sem.at[1 + k]))
        stores[-1].start()
    for copy in started:
        copy.wait_send()
    for k in range(len(CHUNKS)):
        both = pl.ds(starts[k], CHUNKS[k])
        landed(csend.at[both], csend_sem.at[k])
    @pl.when(same)
    def _():
        landed(xr.at[pl.ds(0, 3)], xsend_sem)

    @pl.when(jnp.logical_not(same))
    def _():
        landed(xr, xsend_sem)

    for copy in stores:
        copy.wait()


def layer(weights, cotangents, tokens, gain, down, ups):
    count, owned_width = tokens.shape
    owned = weights[0].shape[0]
    rows = (40, owned - 40)
    width = sum(w.shape[1] for w in weights)
    events = sum(kind == "event" for kind, _, _ in make_plan(rows, TASKS)[1])
    slots = 2 * NY * NZ
    chunks = len(CHUNKS)
    rank3 = down.shape[0]
    f32, bf16, dma = jnp.float32, jnp.bfloat16, pltpu.SemaphoreType.DMA
    return pl.pallas_call(
        functools.partial(layer_kernel, rows),
        out_shape=(
            jax.ShapeDtypeStruct((count, owned_width), bf16),
            jax.ShapeDtypeStruct((AR_USED, 2, 16, 128), f32),
        ),
        in_specs=[pl.BlockSpec(memory_space=pltpu.HBM)] * 12,
        out_specs=(pl.BlockSpec(memory_space=pl.ANY),) * 2,
        scratch_shapes=[
            pltpu.VMEM((slots, SLOT, width), bf16),
            pltpu.VMEM((2 * count, width), bf16),
            pltpu.VMEM((slots * SLOT, count), f32),
            pltpu.VMEM((slots, SLOT, count), bf16),
            pltpu.VMEM((slots, SLOT, count), bf16),
            pltpu.VMEM((slots, SLOT, count), bf16),
            pltpu.VMEM((4, NZ, owned, count), bf16),
            *(pltpu.VMEM(a.shape, a.dtype) for a in (gain, down, *ups)),
            pltpu.VMEM((count, owned_width), bf16),
            pltpu.VMEM((owned_width, count), f32),
            pltpu.VMEM((owned_width, count), f32),
            pltpu.VMEM((count, owned_width), f32),
            pltpu.VMEM((count, owned_width), bf16),
            pltpu.VMEM((owned_width, 128), f32),
            pltpu.VMEM((4, 2 * rank3 + 16, count), f32),
            pltpu.VMEM((2 * rank3 + 16, count), f32),
            pltpu.VMEM((rank3, count), bf16),
            pltpu.VMEM((8, count), f32),
            pltpu.VMEM((4, 8, count), f32),
            pltpu.VMEM((NY * NZ, 2, 16, 128), f32),
            pltpu.VMEM((AR_USED, 16, 128), f32),
            pltpu.VMEM((NY - 1, NZ, 16, 128), f32),
            pltpu.VMEM((NZ - 1, 16, 128), f32),
            pltpu.VMEM((NY * NZ, 2, 16, 128), f32),
            dma((15,)), dma((events,)), dma((events,)), dma((G_PIECES,)), dma((G_PIECES,)),
            dma((chunks,)), dma((chunks,)), dma, dma((4,)),
            dma((3,)), dma((3,)), dma((22,)), dma((22,)), dma((3,)), dma((3,)), dma((1 + OUT_PIECES,)),
        ],
        compiler_params=pltpu.CompilerParams(collective_id=0, has_side_effects=True, vmem_limit_bytes=VMEM_LIMIT),
        cost_estimate=pl.CostEstimate(flops=9 * 10**9, bytes_accessed=6 * 10**6, transcendentals=0),
        name="layer",
    )(*(pltpu.with_memory_space_constraint(a, pltpu.HBM) for a in (*weights, *cotangents, tokens, gain, down, *ups)))


def finish_kernel(grad_in, adapter_in, grad, down, upq, upk, upv, adapter, sem):
    load = pltpu.make_async_copy(adapter_in, adapter, sem.at[0])
    load.start()
    store = pltpu.make_async_copy(grad_in, grad, sem.at[1])
    store.start()
    load.wait()
    at = 0
    for ref in (down, upq, upk, upv):
        for j in range(ref.shape[1] // 128):
            for k in range(ref.shape[0] // 16):
                ref[k * 16 : (k + 1) * 16, j * 128 : (j + 1) * 128] = adapter[at // 2, at % 2]
                at += 1
    store.wait()


def finish(grad, adapter, rank3, ups):
    f32 = jnp.float32
    shapes = [(rank3, grad.shape[1])] + [u.shape for u in ups]
    vmem = pl.BlockSpec(memory_space=pltpu.VMEM)
    hbm = pl.BlockSpec(memory_space=pl.ANY)
    return pl.pallas_call(
        finish_kernel,
        out_shape=(jax.ShapeDtypeStruct(grad.shape, grad.dtype), *(jax.ShapeDtypeStruct(s, f32) for s in shapes)),
        in_specs=[hbm, hbm],
        out_specs=(hbm, *(vmem,) * 4),
        scratch_shapes=[pltpu.VMEM(adapter.shape, f32), pltpu.SemaphoreType.DMA((2,))],
        compiler_params=pltpu.CompilerParams(vmem_limit_bytes=16 << 20),
        name="finish",
    )(grad, adapter)


def shards(
    tokens,
    gain,
    query_projection_weight,
    key_projection_weight,
    value_projection_weight,
    adapter_down_factors,
    query_adapter_up,
    key_adapter_up,
    value_adapter_up,
    query_cotangent,
    key_cotangent,
    value_cotangent,
):
    kinds, rank, full_width = adapter_down_factors.shape
    ups = (query_adapter_up, key_adapter_up, value_adapter_up)
    grad_tokens, adapter = layer(
        (query_projection_weight, key_projection_weight, value_projection_weight),
        (query_cotangent, key_cotangent, value_cotangent),
        tokens,
        gain.reshape(-1, 128),
        adapter_down_factors.reshape(kinds * rank, full_width),
        ups,
    )
    grad_tokens, grad_down, *grad_ups = finish(grad_tokens, adapter, kinds * rank, ups)
    return (grad_tokens, grad_down.reshape(kinds, rank, -1), *grad_ups)


def solution(mesh):
    in_specs = (
        P("fsdp", "tp"),
        P(),
        P("fsdp", "tp"),
        P("fsdp", "tp"),
        P("fsdp", "tp"),
        P(),
        P(None, "tp"),
        P(None, "tp"),
        P(None, "tp"),
        P("fsdp", "tp"),
        P("fsdp", "tp"),
        P("fsdp", "tp"),
    )
    out_specs = (P("fsdp", "tp"), P(None, None, "tp"), P(None, "tp"), P(None, "tp"), P(None, "tp"))
    return jax.shard_map(shards, mesh=mesh, in_specs=in_specs, out_specs=out_specs, check_vma=False)
```
